32 devices in a mesh: stream: 8 (over y, x, core), cross: 4 (over z).
Axes of the slice: x: 2, y: 2, z: 4, core: 2. Of those that a mesh axis runs over, the one named last changes fastest.
Arguments:
- latents: bfloat16 [16384, 128], P(('stream', 'cross')), may hold values from -6 to 6
- stale_latents: bfloat16 [16384, 128], P(('stream', 'cross')), may hold values from -6 to 6
- edge_latents: bfloat16 [49152, 128], P(('stream', 'cross')), may hold values from -6 to 6
- senders: int32 [49152], P(('stream', 'cross')), may hold values from 0 to 1023
- receivers: int32 [49152], P(('stream', 'cross')), may hold values from 0 to 511
- edge_count: int32 [32], P(('stream', 'cross')), may hold values from 512 to 1536, as said below
- send_list: int32 [32, 4, 128], P(('stream', 'cross')), may hold values from 0 to 511
- node_cotangent: bfloat16 [16384, 128], P(('stream', 'cross')), may hold values from -6 to 6
- edge_cotangent: bfloat16 [49152, 128], P(('stream', 'cross')), may hold values from -6 to 6
- edge_first: bfloat16 [384, 128], replicated, may hold values from -0.3125 to 0.3125
- edge_bias: float32 [128], replicated, may hold values from -3 to 3
- edge_second: bfloat16 [128, 128], replicated, may hold values from -0.5 to 0.5
- edge_gain: float32 [128], replicated, may hold values from 0.25 to 1.75
- node_first: bfloat16 [256, 128], replicated, may hold values from -0.375 to 0.375
- node_bias: float32 [128], replicated, may hold values from -3 to 3
- node_second: bfloat16 [128, 128], replicated, may hold values from -0.5 to 0.5
- node_gain: float32 [128], replicated, may hold values from 0.25 to 1.75
Outputs:
- new_latents: bfloat16 [16384, 128], P(('stream', 'cross'))
- latent_grads: bfloat16 [16384, 128], P(('stream', 'cross'))
- stale_grads: bfloat16 [16384, 128], P(('stream', 'cross'))
- edge_grads: bfloat16 [49152, 128], P(('stream', 'cross'))
- edge_first_grad: float32 [384, 128], replicated
- edge_bias_grad: float32 [128], replicated
- edge_second_grad: float32 [128, 128], replicated
- edge_gain_grad: float32 [128], replicated
- node_first_grad: float32 [256, 128], replicated
- node_bias_grad: float32 [128], replicated
- node_second_grad: float32 [128, 128], replicated
- node_gain_grad: float32 [128], replicated
The draws below stay inside these ranges and needn't reach their ends.
Inputs may be any that keep to these rules, and one draw needn't show every extreme that they name: `edge_count`: a partition's live edge slots come first; some partition has 1536 live slots. `senders`: rows below 512 are the partition's own nodes, the rest its four halo blocks in the order of the steps. `send_list`: a row may be listed more than once.
All inputs are finite; a program needn't handle non-finite values.
Results may differ from the reference program's by a relative error of at most 0.015.
Values may be sent and summed in bfloat16 or wider, within the bound.
No kernel may reach another device: no remote copies, remote signals or barrier semaphores. Data moves between devices by JAX's collectives and lax.ppermute only.
A program may use at most 64 MiB of HBM per device.

```python
import math
import jax
import jax.numpy as jnp
from jax import lax

WIDTH = 128
NODES_DEV = 512
HALO = 128
EDGES_DEV = 1536
NODES = 16384
EDGES = 49152
N_STREAM = 8
N_CROSS = 4
DEVICES = 32


def draw_edge_count(key, part):
    first_key, second_key = jax.random.split(jax.random.fold_in(key, 11))
    counts = jax.random.randint(first_key, (DEVICES,), EDGES_DEV // 3, EDGES_DEV + 1)
    chosen = jax.random.randint(second_key, (), 0, DEVICES)
    return jnp.where(jnp.arange(DEVICES) == chosen, EDGES_DEV, counts).astype(jnp.int32)


def set_ends(values, key, smallest, top_value):
    spot = [jax.random.randint(jax.random.fold_in(key, axis), (), 0, length) for axis, length in enumerate(values.shape)]
    longest = values.shape.index(max(values.shape))
    neighbour = spot[:longest] + [(spot[longest] + 1) % values.shape[longest]] + spot[longest + 1:]
    return values.at[tuple(spot)].set(smallest).at[tuple(neighbour)].set(top_value)


def level_of(stream_key, shape, pieces, smallest, top_value):
    factor_of = 1.0
    for position, shards_of in pieces:
        draws = jax.random.uniform(jax.random.fold_in(jax.random.fold_in(stream_key, 6), position), (shards_of,), jnp.float32, smallest / len(pieces), top_value / len(pieces))
        factor_of = factor_of * jnp.repeat(jnp.exp(draws), shape[position] // shards_of).reshape((-1,) + (1,) * (len(shape) - 1 - position))
    return factor_of


def noise(rng, dims, spread, most, pieces=(), held_as=jnp.bfloat16):
    result = spread * jax.random.normal(rng, dims, jnp.float32)
    if pieces:
        result = result * level_of(rng, dims, pieces, -0.22, 0.18)
    return jnp.clip(result, -most, most).astype(held_as)


def setup_inputs(seed: int = 0) -> dict:
    keys = jax.random.split(jax.random.key(seed), 18)
    latents = noise(keys[0], (NODES, WIDTH), 1.0, 6.0, ((0, 32),))
    stale_latents = noise(keys[1], (NODES, WIDTH), 1.0, 6.0, ((0, 32),))
    edge_latents = noise(keys[2], (EDGES, WIDTH), 1.0, 6.0, ((0, 32),))
    senders = set_ends(jax.random.randint(keys[3], (EDGES,), 0, NODES_DEV + 4 * HALO), jax.random.fold_in(keys[3], 1), 0, (NODES_DEV + 4 * HALO) - 1).astype(jnp.int32)
    receivers = set_ends(jax.random.randint(keys[4], (EDGES,), 0, NODES_DEV), jax.random.fold_in(keys[4], 1), 0, NODES_DEV - 1).astype(jnp.int32)
    edge_count = draw_edge_count(jax.random.fold_in(keys[17], 71), 0)
    send_list = set_ends(jax.random.randint(keys[6], (DEVICES, 4, HALO), 0, NODES_DEV), jax.random.fold_in(keys[6], 1), 0, NODES_DEV - 1).astype(jnp.int32)
    node_cotangent = noise(keys[7], (NODES, WIDTH), 1.0, 6.0, ((0, 32),))
    edge_cotangent = noise(keys[8], (EDGES, WIDTH), 1.0, 6.0, ((0, 32),))
    edge_first = noise(keys[9], (3 * WIDTH, WIDTH), (3 * WIDTH) ** -0.5, 0.3125)
    edge_bias = noise(keys[10], (WIDTH,), 0.5, 3.0, (), jnp.float32)
    edge_second = noise(keys[11], (WIDTH, WIDTH), WIDTH ** -0.5, 0.5)
    edge_gain = jnp.clip(1.0 + 0.15 * jax.random.normal(keys[12], (WIDTH,), jnp.float32), 0.25, 1.75)
    node_first = noise(keys[13], (2 * WIDTH, WIDTH), (2 * WIDTH) ** -0.5, 0.375)
    node_bias = noise(keys[14], (WIDTH,), 0.5, 3.0, (), jnp.float32)
    node_second = noise(keys[15], (WIDTH, WIDTH), WIDTH ** -0.5, 0.5)
    node_gain = jnp.clip(1.0 + 0.15 * jax.random.normal(keys[16], (WIDTH,), jnp.float32), 0.25, 1.75)
    return {"latents": latents, "stale_latents": stale_latents, "edge_latents": edge_latents, "senders": senders, "receivers": receivers, "edge_count": edge_count, "send_list": send_list, "node_cotangent": node_cotangent, "edge_cotangent": edge_cotangent, "edge_first": edge_first, "edge_bias": edge_bias, "edge_second": edge_second, "edge_gain": edge_gain, "node_first": node_first, "node_bias": node_bias, "node_second": node_second, "node_gain": node_gain}


EPSILON = 1e-05

def layer_norm(values, scale_gain):
    row_mean = lax.optimization_barrier(jnp.mean(values, axis=-1, keepdims=True))
    centered = values - row_mean
    variance = lax.optimization_barrier(jnp.mean(centered * centered, axis=-1, keepdims=True))
    return centered * lax.rsqrt(variance + EPSILON) * scale_gain

def local_layer(owned, halo_rows, edge_rows, params, senders, receivers, edge_total):
    edge_first, edge_bias, edge_second, edge_gain, node_first, node_bias, node_second, node_gain = params
    node_table = jnp.concatenate([owned, halo_rows], axis=0)
    sender_rows = jnp.take(node_table, senders, axis=0)
    receiver_rows = jnp.take(owned, receivers, axis=0)
    joined = jnp.concatenate([edge_rows, sender_rows, receiver_rows], axis=1).astype(jnp.bfloat16)
    hidden_pre = jnp.dot(joined, edge_first, preferred_element_type=jnp.float32) + edge_bias
    edge_hidden = jax.nn.silu(hidden_pre).astype(jnp.bfloat16)
    edge_out = jnp.dot(edge_hidden, edge_second, preferred_element_type=jnp.float32)
    edge_alive = (jnp.arange(edge_rows.shape[0], dtype=jnp.int32) < edge_total).astype(jnp.float32)[:, None]
    new_edges = (edge_rows + edge_alive * layer_norm(edge_out, edge_gain)).astype(jnp.bfloat16)
    summed = jnp.zeros(owned.shape, jnp.float32).at[receivers].add(edge_alive * new_edges.astype(jnp.float32))
    node_input = jnp.concatenate([owned, summed], axis=1).astype(jnp.bfloat16)
    node_pre = jnp.dot(node_input, node_first, preferred_element_type=jnp.float32) + node_bias
    node_hidden = jax.nn.silu(node_pre).astype(jnp.bfloat16)
    node_out = jnp.dot(node_hidden, node_second, preferred_element_type=jnp.float32)
    new_latents = (owned + layer_norm(node_out, node_gain)).astype(jnp.bfloat16)
    return (new_latents, new_edges)

def local_step(latent_block, halo_block, edge_block, params, senders, receivers, edge_total, node_cot, edge_cot):

    def forward(owned, halo_rows, edge_rows, weights):
        return local_layer(owned, halo_rows, edge_rows, weights, senders, receivers, edge_total)
    outputs, pullback = jax.vjp(forward, latent_block.astype(jnp.float32), halo_block.astype(jnp.float32), edge_block.astype(jnp.float32), params)
    grad_owned, grad_halo, grad_edges, grad_params = pullback((node_cot.astype(outputs[0].dtype), edge_cot.astype(outputs[1].dtype)))
    grad_params = tuple((item.astype(jnp.float32) for item in grad_params))
    return (outputs[0], grad_owned, grad_halo, grad_edges, grad_params)

def reference(latents, stale_latents, edge_latents, senders, receivers, edge_count, send_list, node_cotangent, edge_cotangent, edge_first, edge_bias, edge_second, edge_gain, node_first, node_bias, node_second, node_gain):
    rows_s = N_STREAM
    rows_c = N_CROSS
    width = latents.shape[1]
    parts = rows_s * rows_c
    owned_all = latents.reshape(parts, NODES_DEV, width)
    stale_all = stale_latents.reshape(parts, NODES_DEV, width)
    send_rows = send_list.reshape(parts, 4 * HALO)
    picked = jax.vmap(lambda table, index: jnp.take(table, index, axis=0))(stale_all, send_rows)
    picked = picked.reshape(rows_s, rows_c, 4, HALO, width)
    zeros_s = jnp.zeros((1, rows_c, HALO, width), picked.dtype)
    zeros_c = jnp.zeros((rows_s, 1, HALO, width), picked.dtype)
    block_zero = jnp.concatenate([zeros_s, picked[:-1, :, 0]], axis=0)
    block_one = jnp.concatenate([picked[1:, :, 1], zeros_s], axis=0)
    block_two = jnp.concatenate([zeros_c, picked[:, :-1, 2]], axis=1)
    block_three = jnp.concatenate([picked[:, 1:, 3], zeros_c], axis=1)
    halo_all = jnp.stack([block_zero, block_one, block_two, block_three], axis=2).reshape(parts, 4 * HALO, width)
    params = (edge_first, edge_bias, edge_second, edge_gain, node_first, node_bias, node_second, node_gain)

    def one_part(items):
        owned, halo_rows, edge_rows, send_idx, recv_idx, edge_total, node_cot, edge_cot = items
        return local_step(owned, halo_rows, edge_rows, params, send_idx, recv_idx, edge_total, node_cot, edge_cot)
    items = (owned_all, halo_all, edge_latents.reshape(parts, EDGES_DEV, width), senders.reshape(parts, EDGES_DEV), receivers.reshape(parts, EDGES_DEV), edge_count, node_cotangent.reshape(parts, NODES_DEV, width), edge_cotangent.reshape(parts, EDGES_DEV, width))
    new_latents, grad_owned, grad_halo, grad_edges, grad_params = lax.map(one_part, items)
    halo_grads = grad_halo.reshape(rows_s, rows_c, 4, HALO, width)
    fzero_s = jnp.zeros((1, rows_c, HALO, width), jnp.float32)
    fzero_c = jnp.zeros((rows_s, 1, HALO, width), jnp.float32)
    back_zero = jnp.concatenate([halo_grads[1:, :, 0], fzero_s], axis=0)
    back_one = jnp.concatenate([fzero_s, halo_grads[:-1, :, 1]], axis=0)
    back_two = jnp.concatenate([halo_grads[:, 1:, 2], fzero_c], axis=1)
    back_three = jnp.concatenate([fzero_c, halo_grads[:, :-1, 3]], axis=1)
    returned = jnp.stack([back_zero, back_one, back_two, back_three], axis=2).reshape(parts, 4 * HALO, width)
    stale_grads = jax.vmap(lambda index, values: jnp.zeros((NODES_DEV, width), jnp.float32).at[index].add(values))(send_rows, returned)
    totals = tuple((lax.optimization_barrier(jnp.sum(item, axis=0)) for item in grad_params))
    squares = jnp.zeros((), jnp.float32)
    entries = 0
    for item in totals:
        squares = squares + jnp.sum(item * item)
        entries = entries + item.size
    factor = jnp.minimum(1.0, math.sqrt(entries) * lax.rsqrt(squares))
    clipped = tuple((item * factor for item in totals))
    return (new_latents.reshape(parts * NODES_DEV, width), grad_owned.astype(jnp.bfloat16).reshape(parts * NODES_DEV, width), stale_grads.astype(jnp.bfloat16).reshape(parts * NODES_DEV, width), grad_edges.astype(jnp.bfloat16).reshape(parts * EDGES_DEV, width), clipped[0], clipped[1], clipped[2], clipped[3], clipped[4], clipped[5], clipped[6], clipped[7])
```

```python
import functools
import math

import jax
import jax.numpy as jnp
from jax import lax
from jax.experimental import pallas as pl
from jax.experimental.pallas import tpu as pltpu
from jax.sharding import PartitionSpec as P

EPSILON = 1e-05
BF = jnp.bfloat16
F32 = jnp.float32
VMEM_LIMIT = 40 * 1024 * 1024


def mm(a, b):
    return jnp.dot(a, b, preferred_element_type=F32)


def mm_nt(a, b):
    return lax.dot_general(a, b, (((1,), (1,)), ((), ())), preferred_element_type=F32)


def mm_tn(a, b):
    return lax.dot_general(a, b, (((0,), (0,)), ((), ())), preferred_element_type=F32)


def index_columns(index_ref, row):
    line = index_ref[row : row + 1, :].astype(F32)
    return jnp.broadcast_to(line, (line.shape[1], line.shape[1])).T


def one_hot_rows(column, size):
    lanes = column.shape[1]
    lane = lax.broadcasted_iota(jnp.int32, column.shape, 1).astype(F32)
    blocks = [
        jnp.where(column == lane + float(base), 1.0, 0.0).astype(BF)
        for base in range(0, size, lanes)
    ]
    return jnp.concatenate(blocks, axis=1)


def one_hot_columns(index_ref, row, size):
    line = index_ref[row : row + 1, :]
    place = lax.broadcasted_iota(jnp.int32, (size, line.shape[1]), 0)
    return jnp.where(place == line, 1.0, 0.0).astype(BF)


def pick_kernel(list_ref, stale_ref, out_ref):
    width = list_ref.shape[1]
    for block in range(list_ref.shape[0]):
        hot = one_hot_rows(index_columns(list_ref, block), stale_ref.shape[0])
        out_ref[block] = mm(hot, stale_ref[...]).astype(BF)


def stale_kernel(list_ref, b0, b1, b2, b3, out_ref):
    total = None
    for block, part in enumerate((b0, b1, b2, b3)):
        hot = one_hot_columns(list_ref, block, out_ref.shape[0])
        piece = mm(hot, part[...])
        total = piece if total is None else total + piece
    out_ref[...] = total.astype(BF)


def norm_forward(z):
    mean = jnp.mean(z, axis=-1, keepdims=True)
    centered = z - mean
    variance = jnp.mean(centered * centered, axis=-1, keepdims=True)
    inverse = lax.rsqrt(variance + EPSILON)
    return centered * inverse, jnp.broadcast_to(inverse, z.shape)


def norm_backward(slope, unit, inverse):
    first = jnp.mean(slope, axis=-1, keepdims=True)
    second = jnp.mean(slope * unit, axis=-1, keepdims=True)
    return inverse * (slope - first - unit * second)


def silu_pair(v):
    sig = 1.0 / (1.0 + jnp.exp(-v))
    hidden = v * sig
    return hidden, sig + hidden * (1.0 - sig)


def main_kernel(
    count_ref,
    latents,
    h0,
    h1,
    h2,
    h3,
    edges,
    senders,
    receivers,
    node_cot,
    edge_cot,
    edge_first,
    edge_bias,
    edge_second,
    edge_gain,
    node_first,
    node_bias,
    node_second,
    node_gain,
    new_latents,
    latent_grads,
    edge_grads,
    halo_grads,
    packed,
    table,
    hot_recv,
    turn_recv,
    turn_send,
    send_rows,
    recv_rows,
    hidden_s,
    slope_s,
    unit_s,
    inverse_s,
    alive_edges,
    dz_s,
    dpre_s,
):
    n, w = latents.shape
    e = edges.shape[0]
    t = table.shape[0]
    depth = h0.shape[0]
    total = count_ref[0]
    chunk = 2 * w
    table[:n] = latents[...]
    for i, part in enumerate((h0, h1, h2, h3)):
        table[n + i * depth : n + (i + 1) * depth] = part[...]
    gain = edge_gain[...]

    for c in range(e // chunk):
        rows = slice(c * chunk, (c + 1) * chunk)
        for b in range(chunk // w):
            row = c * (chunk // w) + b
            part = slice(row * w, (row + 1) * w)
            hot = one_hot_rows(index_columns(senders, row), t)
            send_rows[part] = mm(hot, table[...]).astype(BF)
            hot = one_hot_rows(index_columns(receivers, row), n)
            hot_recv[part] = hot
            recv_rows[part] = mm(hot, latents[...]).astype(BF)
            turn_send[:, part] = one_hot_columns(senders, row, t)
            turn_recv[:, part] = one_hot_columns(receivers, row, n)
        edge = edges[rows]
        pre = (
            mm(edge, edge_first[:w])
            + mm(send_rows[rows], edge_first[w : 2 * w])
            + mm(recv_rows[rows], edge_first[2 * w :])
            + edge_bias[...]
        )
        hidden, slope = silu_pair(pre)
        hidden = hidden.astype(BF)
        hidden_s[rows] = hidden
        slope_s[rows] = slope
        unit, inverse = norm_forward(mm(hidden, edge_second[...]))
        unit_s[rows] = unit
        inverse_s[rows] = inverse
        place = lax.broadcasted_iota(jnp.int32, (chunk, w), 0) + c * chunk
        fresh = (edge.astype(F32) + unit * gain).astype(BF)
        alive_edges[rows] = jnp.where(place < total, fresh, jnp.zeros_like(fresh))

    aggregate = mm(turn_recv[...], alive_edges[...]).astype(BF)
    own = latents[...]
    hidden, slope = silu_pair(mm(own, node_first[:w]) + mm(aggregate, node_first[w:]) + node_bias[...])
    hidden = hidden.astype(BF)
    unit, inverse = norm_forward(mm(hidden, node_second[...]))
    new_latents[...] = (own.astype(F32) + unit * node_gain[...]).astype(BF)
    ncot = node_cot[...].astype(F32)
    node_gain_grad = jnp.sum(ncot * unit, axis=0, keepdims=True)
    dz = norm_backward(ncot * node_gain[...], unit, inverse).astype(BF)
    dpre = mm_nt(dz, node_second[...]) * slope
    node_bias_grad = jnp.sum(dpre, axis=0, keepdims=True)
    dpre = dpre.astype(BF)
    d_aggregate = mm_nt(dpre, node_first[w:]).astype(BF)
    latent_part = ncot + mm_nt(dpre, node_first[:w])
    at = 4 * w
    packed[at : at + w] = mm_tn(own, dpre).astype(BF)
    packed[at + w : at + 2 * w] = mm_tn(aggregate, dpre).astype(BF)
    packed[at + 2 * w : at + 3 * w] = mm_tn(hidden, dz).astype(BF)

    bias_grad = jnp.zeros((1, w), F32)
    gain_grad = jnp.zeros((1, w), F32)
    for c in range(e // chunk):
        rows = slice(c * chunk, (c + 1) * chunk)
        place = lax.broadcasted_iota(jnp.int32, (chunk, w), 0) + c * chunk
        alive = place < total
        passed = mm(hot_recv[rows], d_aggregate)
        cot = edge_cot[rows].astype(F32) + jnp.where(alive, passed, 0.0)
        live = jnp.where(alive, cot, 0.0)
        unit = unit_s[rows]
        gain_grad = gain_grad + jnp.sum(live * unit, axis=0, keepdims=True)
        dz = norm_backward(live * gain, unit, inverse_s[rows]).astype(BF)
        dz_s[rows] = dz
        dpre = mm_nt(dz, edge_second[...]) * slope_s[rows]
        bias_grad = bias_grad + jnp.sum(dpre, axis=0, keepdims=True)
        dpre = dpre.astype(BF)
        dpre_s[rows] = dpre
        edge_grads[rows] = (cot + mm_nt(dpre, edge_first[:w])).astype(BF)

    dpre = dpre_s[...]
    packed[:w] = mm_tn(edges[...], dpre).astype(BF)
    packed[w : 2 * w] = mm_tn(send_rows[...], dpre).astype(BF)
    packed[2 * w : 3 * w] = mm_tn(recv_rows[...], dpre).astype(BF)
    packed[3 * w : 4 * w] = mm_tn(hidden_s[...], dz_s[...]).astype(BF)
    tail = jnp.concatenate(
        [bias_grad, gain_grad, node_bias_grad, node_gain_grad, jnp.zeros((w - 4, w), F32)], axis=0
    )
    packed[7 * w :] = tail.astype(BF)

    from_send = mm(turn_send[...], dpre).astype(BF)
    from_recv = mm(turn_recv[...], dpre).astype(BF)
    back = mm_nt(from_send, edge_first[w : 2 * w])
    latent_grads[...] = (
        latent_part + back[:n] + mm_nt(from_recv, edge_first[2 * w :])
    ).astype(BF)
    halo_grads[...] = back[n:].astype(BF)


def final_kernel(limit, bit_ref, mine, other, *outs):
    swap = bit_ref[0] == 1
    a, b = (mine[...].astype(F32), other[...].astype(F32))
    low = jnp.where(swap, b, a)
    high = jnp.where(swap, a, b)
    squares = jnp.sum(a * a + b * b)
    factor = jnp.minimum(1.0, limit * lax.rsqrt(jnp.full((1, a.shape[1]), squares, F32)))
    w = a.shape[1]
    full = (low * factor, high * factor)
    ef, eb, es, eg, nf, nb, ns, ng = outs
    half = 4 * w
    ef[...] = full[0][: 3 * w]
    es[...] = full[0][3 * w :]
    nf[...] = full[1][: 2 * w]
    ns[...] = full[1][2 * w : 3 * w]
    eb[...] = full[1][3 * w : 3 * w + 1]
    eg[...] = full[1][3 * w + 1 : 3 * w + 2]
    nb[...] = full[1][3 * w + 2 : 3 * w + 3]
    ng[...] = full[1][3 * w + 3 : 3 * w + 4]


VM = pl.BlockSpec(memory_space=pltpu.VMEM)
SM = pl.BlockSpec(memory_space=pltpu.SMEM)


def call(kernel, outs, scratch=(), specs=None, name=None):
    return pl.pallas_call(
        kernel,
        out_shape=outs,
        in_specs=specs,
        out_specs=jax.tree.map(lambda _: VM, outs),
        scratch_shapes=list(scratch),
        compiler_params=pltpu.CompilerParams(vmem_limit_bytes=VMEM_LIMIT),
        name=name,
    )


def flip(axis, bit):
    return [(i, i ^ bit) for i in range(lax.axis_size(axis))]


def pair_sum(parts):
    parts = [p.astype(F32) for p in parts]
    while len(parts) > 1:
        parts = [parts[i] + parts[i + 1] for i in range(0, len(parts), 2)]
    return parts[0].astype(BF)


def exchange(value, axis, bits):
    out = [value]
    for m in range(1, 1 << len(bits)):
        mask = sum(bits[j] for j in range(len(bits)) if m >> j & 1)
        out.append(lax.ppermute(value, axis, flip(axis, mask)))
    return out


def scatter_sum(value, axis, low, radix):
    spot = (lax.axis_index(axis) // low) % radix
    blocks = value.reshape((radix, value.shape[0] // radix) + value.shape[1:])
    got = []
    for k in range(radix):
        block = lax.dynamic_index_in_dim(blocks, spot ^ k, 0, False)
        got.append(block if k == 0 else lax.ppermute(block, axis, flip(axis, k * low)))
    return pair_sum(got)


def gather_back(value, axis, low, radix):
    spot = (lax.axis_index(axis) // low) % radix
    got = [value] + [lax.ppermute(value, axis, flip(axis, k * low)) for k in range(1, radix)]
    stack = jnp.stack(got)
    return jnp.concatenate(
        [lax.dynamic_index_in_dim(stack, spot ^ k, 0, False) for k in range(radix)], axis=0
    )


def reduce_rest(value):
    stream, cross = (lax.axis_size("stream"), lax.axis_size("cross"))
    value = scatter_sum(value, "stream", 2, 4)
    low = 8
    while low < stream:
        value = pair_sum(exchange(value, "stream", [low]))
        low *= 2
    low = 1
    while low < cross:
        value = pair_sum(exchange(value, "cross", [low, 2 * low] if 2 * low < cross else [low]))
        low *= 4
    return gather_back(value, "stream", 2, 4)


def shift(value, axis, step):
    size = lax.axis_size(axis)
    pairs = [(i, i + step) for i in range(size) if 0 <= i + step < size]
    return lax.ppermute(value, axis, pairs)


def per_device(
    latents,
    stale_latents,
    edge_latents,
    senders,
    receivers,
    edge_count,
    send_list,
    node_cotangent,
    edge_cotangent,
    edge_first,
    edge_bias,
    edge_second,
    edge_gain,
    node_first,
    node_bias,
    node_second,
    node_gain,
):
    n, w = latents.shape
    e = edge_latents.shape[0]
    depth = send_list.shape[2]
    lists = send_list[0]
    picked = call(
        pick_kernel, jax.ShapeDtypeStruct((4, depth, w), BF), specs=[VM, VM], name="pick"
    )(lists, stale_latents)
    halo = (
        shift(picked[0], "stream", 1),
        shift(picked[1], "stream", -1),
        shift(picked[2], "cross", 1),
        shift(picked[3], "cross", -1),
    )
    table = n + 4 * depth

    def shape(rows, kind=BF):
        return jax.ShapeDtypeStruct((rows, w), kind)

    new_latents, latent_grads, edge_grads, halo_grads, packed = call(
        main_kernel,
        (shape(n), shape(n), shape(e), shape(4 * depth), shape(8 * w)),
        scratch=(
            pltpu.VMEM((table, w), BF),
            pltpu.VMEM((e, n), BF),
            pltpu.VMEM((n, e), BF),
            pltpu.VMEM((table, e), BF),
            pltpu.VMEM((e, w), BF),
            pltpu.VMEM((e, w), BF),
            pltpu.VMEM((e, w), BF),
            pltpu.VMEM((e, w), F32),
            pltpu.VMEM((e, w), F32),
            pltpu.VMEM((e, w), F32),
            pltpu.VMEM((e, w), BF),
            pltpu.VMEM((e, w), BF),
            pltpu.VMEM((e, w), BF),
        ),
        specs=[SM] + [VM] * 18,
        name="layer",
    )(
        edge_count,
        latents,
        *halo,
        edge_latents,
        senders.reshape(e // w, w),
        receivers.reshape(e // w, w),
        node_cotangent,
        edge_cotangent,
        edge_first,
        edge_bias.reshape(1, w),
        edge_second,
        edge_gain.reshape(1, w),
        node_first,
        node_bias.reshape(1, w),
        node_second,
        node_gain.reshape(1, w),
    )
    back = halo_grads.reshape(4, depth, w)
    returned = (
        shift(back[0], "stream", -1),
        shift(back[1], "stream", 1),
        shift(back[2], "cross", -1),
        shift(back[3], "cross", 1),
    )
    stale_grads = call(stale_kernel, shape(n), specs=[VM] * 5, name="stale")(lists, *returned)

    bit = lax.axis_index("stream") % 2
    part = reduce_rest(scatter_sum(packed, "stream", 1, 2))
    other = lax.ppermute(part, "stream", flip("stream", 1))
    sizes = (3 * w * w, w, w * w, w, 2 * w * w, w, w * w, w)
    limit = math.sqrt(sum(sizes))
    clipped = call(
        functools.partial(final_kernel, limit),
        tuple(shape(s // w, F32) for s in sizes),
        specs=[SM, VM, VM],
        name="clip",
    )(bit.reshape(1), part, other)
    clipped = tuple(c.reshape(w) if s == w else c for c, s in zip(clipped, sizes))
    return (new_latents, latent_grads, stale_grads, edge_grads) + clipped


def solution(mesh):
    shard = P(("stream", "cross"))
    rows = P(("stream", "cross"), None)
    in_specs = (rows, rows, rows, shard, shard, shard, P(("stream", "cross"), None, None), rows, rows)
    in_specs = in_specs + (P(),) * 8
    out_specs = (rows,) * 4 + (P(),) * 8
    return jax.shard_map(
        per_device, mesh=mesh, in_specs=in_specs, out_specs=out_specs, check_vma=False
    )
```

```python
import functools
import math

import jax
import jax.numpy as jnp
from jax import lax
from jax.experimental import pallas as pl
from jax.experimental.pallas import tpu as pltpu
from jax.sharding import PartitionSpec as P

EPSILON = 1e-05
BF = jnp.bfloat16
F32 = jnp.float32
VMEM_LIMIT = 40 * 1024 * 1024


def mm(a, b):
    return jnp.dot(a, b, preferred_element_type=F32)


def mm_nt(a, b):
    return lax.dot_general(a, b, (((1,), (1,)), ((), ())), preferred_element_type=F32)


def mm_tn(a, b):
    return lax.dot_general(a, b, (((0,), (0,)), ((), ())), preferred_element_type=F32)


def index_columns(index_ref, row):
    line = index_ref[pl.ds(row, 1), :].astype(F32)
    return jnp.broadcast_to(line, (line.shape[1], line.shape[1])).T


def one_hot_rows(column, size):
    lanes = column.shape[1]
    lane = lax.broadcasted_iota(jnp.int32, column.shape, 1).astype(F32)
    blocks = [
        jnp.where(column == lane + float(base), 1.0, 0.0).astype(BF)
        for base in range(0, size, lanes)
    ]
    return jnp.concatenate(blocks, axis=1)


def one_hot_columns(index_ref, row, size):
    line = index_ref[pl.ds(row, 1), :]
    place = lax.broadcasted_iota(jnp.int32, (size, line.shape[1]), 0)
    return jnp.where(place == line, 1.0, 0.0).astype(BF)


def parities():
    return (lax.rem(lax.axis_index("stream"), 2), lax.rem(lax.axis_index("cross"), 2))


def inner(axis):
    place = lax.axis_index(axis)
    return jnp.logical_and(place > 0, place < lax.axis_size(axis) - 1)


def list_order():
    odd_s, odd_c = parities()
    return (odd_s, 1 - odd_s, 2 + odd_c, 3 - odd_c)


def load_kernel(list_hbm, stale_hbm, *rest):
    count = (len(rest) - 4 - 3) // 2
    sources = rest[:count]
    outs = rest[count : count + 4]
    kept = rest[count + 4 : 2 * count + 4]
    lists, stale, sems = rest[2 * count + 4 :]
    copies = [
        pltpu.make_async_copy(a, b, sems.at[i])
        for i, (a, b) in enumerate(
            zip((list_hbm, stale_hbm) + sources, (lists, stale) + kept)
        )
    ]
    for copy in copies:
        copy.start()
    copies[0].wait()
    columns = [index_columns(lists, row) for row in list_order()]
    copies[1].wait()
    for column, out in zip(columns, outs):
        out[...] = mm(one_hot_rows(column, stale.shape[0]), stale[...]).astype(BF)
    for copy in copies[2:]:
        copy.wait()


def stale_kernel(list_ref, b0, b1, b2, b3, out_ref):
    total = None
    keep = (None, inner("stream"), None, inner("cross"))
    for row, part, valid in zip(list_order(), (b0, b1, b2, b3), keep):
        hot = one_hot_columns(list_ref, row, out_ref.shape[0])
        part = part[...]
        if valid is not None:
            part = jnp.where(valid, part, jnp.zeros_like(part))
        piece = mm(hot, part)
        total = piece if total is None else total + piece
    out_ref[...] = total.astype(BF)


def norm_forward(z):
    mean = jnp.mean(z, axis=-1, keepdims=True)
    centered = z - mean
    variance = jnp.mean(centered * centered, axis=-1, keepdims=True)
    inverse = lax.rsqrt(variance + EPSILON)
    return centered * inverse, jnp.broadcast_to(inverse, z.shape)


def norm_backward(slope, unit, inverse):
    first = jnp.mean(slope, axis=-1, keepdims=True)
    second = jnp.mean(slope * unit, axis=-1, keepdims=True)
    return inverse * (slope - first - unit * second)


def silu_pair(v):
    sig = 1.0 / (1.0 + jnp.exp(-v))
    hidden = v * sig
    return hidden, sig + hidden * (1.0 - sig)


def main_kernel(
    count_ref,
    latents,
    h0,
    h1,
    h2,
    h3,
    edges,
    senders,
    receivers,
    node_cot,
    edge_cot,
    edge_first,
    edge_bias,
    edge_second,
    edge_gain,
    node_first,
    node_bias,
    node_second,
    node_gain,
    new_latents,
    latent_grads,
    edge_grads,
    g0,
    g1,
    g2,
    g3,
    packed,
    table,
    hot_recv,
    turn_recv,
    turn_send,
    send_rows,
    recv_rows,
    hidden_s,
    slope_s,
    unit_s,
    inverse_s,
    alive_edges,
    dz_s,
    dpre_s,
):
    n, w = latents.shape
    e = edges.shape[0]
    t = table.shape[0]
    depth = h0.shape[0]
    total = count_ref[0]
    chunk = 2 * w
    table[:n] = latents[...]
    odd_s, odd_c = parities()
    for i, (near, far, odd, axis) in enumerate(
        ((h0, h1, odd_s, "stream"), (h2, h3, odd_c, "cross"))
    ):
        place = lax.axis_index(axis)
        a, b = (near[...], far[...])
        zero = jnp.zeros_like(a)
        before = jnp.where(place > 0, jnp.where(odd == 1, a, b), zero)
        after = jnp.where(place < lax.axis_size(axis) - 1, jnp.where(odd == 1, b, a), zero)
        at = n + 2 * i * depth
        table[at : at + depth] = before
        table[at + depth : at + 2 * depth] = after
    gain = edge_gain[...]

    for c in range(e // chunk):
        rows = slice(c * chunk, (c + 1) * chunk)
        for b in range(chunk // w):
            row = c * (chunk // w) + b
            part = slice(row * w, (row + 1) * w)
            hot = one_hot_rows(index_columns(senders, row), t)
            send_rows[part] = mm(hot, table[...]).astype(BF)
            hot = one_hot_rows(index_columns(receivers, row), n)
            hot_recv[part] = hot
            recv_rows[part] = mm(hot, latents[...]).astype(BF)
            turn_send[:, part] = one_hot_columns(senders, row, t)
            turn_recv[:, part] = one_hot_columns(receivers, row, n)
        edge = edges[rows]
        pre = (
            mm(edge, edge_first[:w])
            + mm(send_rows[rows], edge_first[w : 2 * w])
            + mm(recv_rows[rows], edge_first[2 * w :])
            + edge_bias[...]
        )
        hidden, slope = silu_pair(pre)
        hidden = hidden.astype(BF)
        hidden_s[rows] = hidden
        slope_s[rows] = slope
        unit, inverse = norm_forward(mm(hidden, edge_second[...]))
        unit_s[rows] = unit
        inverse_s[rows] = inverse
        place = lax.broadcasted_iota(jnp.int32, (chunk, w), 0) + c * chunk
        fresh = (edge.astype(F32) + unit * gain).astype(BF)
        alive_edges[rows] = jnp.where(place < total, fresh, jnp.zeros_like(fresh))

    aggregate = mm(turn_recv[...], alive_edges[...]).astype(BF)
    own = latents[...]
    hidden, slope = silu_pair(mm(own, node_first[:w]) + mm(aggregate, node_first[w:]) + node_bias[...])
    hidden = hidden.astype(BF)
    unit, inverse = norm_forward(mm(hidden, node_second[...]))
    new_latents[...] = (own.astype(F32) + unit * node_gain[...]).astype(BF)
    ncot = node_cot[...].astype(F32)
    node_gain_grad = jnp.sum(ncot * unit, axis=0, keepdims=True)
    dz = norm_backward(ncot * node_gain[...], unit, inverse).astype(BF)
    dpre = mm_nt(dz, node_second[...]) * slope
    node_bias_grad = jnp.sum(dpre, axis=0, keepdims=True)
    dpre = dpre.astype(BF)
    d_aggregate = mm_nt(dpre, node_first[w:]).astype(BF)
    latent_part = ncot + mm_nt(dpre, node_first[:w])
    at = 4 * w
    packed[at : at + w] = mm_tn(own, dpre).astype(BF)
    packed[at + w : at + 2 * w] = mm_tn(aggregate, dpre).astype(BF)
    packed[at + 2 * w : at + 3 * w] = mm_tn(hidden, dz).astype(BF)

    bias_grad = jnp.zeros((1, w), F32)
    gain_grad = jnp.zeros((1, w), F32)
    for c in range(e // chunk):
        rows = slice(c * chunk, (c + 1) * chunk)
        place = lax.broadcasted_iota(jnp.int32, (chunk, w), 0) + c * chunk
        alive = place < total
        passed = mm(hot_recv[rows], d_aggregate)
        cot = edge_cot[rows].astype(F32) + jnp.where(alive, passed, 0.0)
        live = jnp.where(alive, cot, 0.0)
        unit = unit_s[rows]
        gain_grad = gain_grad + jnp.sum(live * unit, axis=0, keepdims=True)
        dz = norm_backward(live * gain, unit, inverse_s[rows]).astype(BF)
        dz_s[rows] = dz
        dpre = mm_nt(dz, edge_second[...]) * slope_s[rows]
        bias_grad = bias_grad + jnp.sum(dpre, axis=0, keepdims=True)
        dpre = dpre.astype(BF)
        dpre_s[rows] = dpre
        edge_grads[rows] = (cot + mm_nt(dpre, edge_first[:w])).astype(BF)

    dpre = dpre_s[...]
    packed[:w] = mm_tn(edges[...], dpre).astype(BF)
    packed[w : 2 * w] = mm_tn(send_rows[...], dpre).astype(BF)
    packed[2 * w : 3 * w] = mm_tn(recv_rows[...], dpre).astype(BF)
    packed[3 * w : 4 * w] = mm_tn(hidden_s[...], dz_s[...]).astype(BF)
    tail = jnp.concatenate(
        [bias_grad, gain_grad, node_bias_grad, node_gain_grad, jnp.zeros((w - 4, w), F32)], axis=0
    )
    packed[7 * w :] = tail.astype(BF)

    from_send = mm(turn_send[...], dpre).astype(BF)
    from_recv = mm(turn_recv[...], dpre).astype(BF)
    back = mm_nt(from_send, edge_first[w : 2 * w])
    latent_grads[...] = (
        latent_part + back[:n] + mm_nt(from_recv, edge_first[2 * w :])
    ).astype(BF)
    for i, (near, far, odd) in enumerate(((g0, g1, odd_s), (g2, g3, odd_c))):
        at = n + 2 * i * depth
        before = back[at : at + depth]
        after = back[at + depth : at + 2 * depth]
        near[...] = jnp.where(odd == 1, before, after).astype(BF)
        far[...] = jnp.where(odd == 1, after, before).astype(BF)


def final_kernel(limit, mine, other, *outs):
    swap = half_of("stream") == 1
    a, b = (mine[...].astype(F32), other[...].astype(F32))
    low = jnp.where(swap, b, a)
    high = jnp.where(swap, a, b)
    squares = jnp.sum(a * a + b * b)
    factor = jnp.minimum(1.0, limit * lax.rsqrt(jnp.full((1, a.shape[1]), squares, F32)))
    w = a.shape[1]
    full = (low * factor, high * factor)
    ef, eb, es, eg, nf, nb, ns, ng = outs
    half = 4 * w
    ef[...] = full[0][: 3 * w]
    es[...] = full[0][3 * w :]
    nf[...] = full[1][: 2 * w]
    ns[...] = full[1][2 * w : 3 * w]
    eb[...] = full[1][3 * w : 3 * w + 1]
    eg[...] = full[1][3 * w + 1 : 3 * w + 2]
    nb[...] = full[1][3 * w + 2 : 3 * w + 3]
    ng[...] = full[1][3 * w + 3 : 3 * w + 4]


VM = pl.BlockSpec(memory_space=pltpu.VMEM)
SM = pl.BlockSpec(memory_space=pltpu.SMEM)
HB = pl.BlockSpec(memory_space=pltpu.HBM)


def call(kernel, outs, scratch=(), specs=None, name=None):
    return pl.pallas_call(
        kernel,
        out_shape=outs,
        in_specs=specs,
        out_specs=jax.tree.map(lambda _: VM, outs),
        scratch_shapes=list(scratch),
        compiler_params=pltpu.CompilerParams(vmem_limit_bytes=VMEM_LIMIT),
        name=name,
    )


def flip(axis, bit):
    return [(i, i ^ bit) for i in range(lax.axis_size(axis))]


def pair_sum(parts):
    parts = [p.astype(F32) for p in parts]
    while len(parts) > 1:
        parts = [parts[i] + parts[i + 1] for i in range(0, len(parts), 2)]
    return parts[0].astype(BF)


def exchange(value, axis, bits):
    out = [value]
    for m in range(1, 1 << len(bits)):
        mask = sum(bits[j] for j in range(len(bits)) if m >> j & 1)
        out.append(lax.ppermute(value, axis, flip(axis, mask)))
    return out


def scatter_sum(value, axis, masks, spot):
    radix = len(masks) + 1
    blocks = value.reshape((radix, value.shape[0] // radix) + value.shape[1:])
    got = [lax.dynamic_index_in_dim(blocks, spot, 0, False)]
    for k, mask in enumerate(masks):
        block = lax.dynamic_index_in_dim(blocks, spot ^ (k + 1), 0, False)
        got.append(lax.ppermute(block, axis, flip(axis, mask)))
    return got


def gather_back(value, axis, masks, spot):
    stack = jnp.stack([value] + [lax.ppermute(value, axis, flip(axis, m)) for m in masks])
    return jnp.concatenate(
        [lax.dynamic_index_in_dim(stack, spot ^ k, 0, False) for k in range(len(masks) + 1)],
        axis=0,
    )


QUAD = (3, 4, 7)


def half_of(axis):
    place = lax.axis_index(axis)
    return lax.rem(place, 2) ^ lax.rem(place // 2, 2)


def quarter_of(axis):
    return lax.rem(lax.axis_index(axis) // 2, 4)


def together(first, second):
    return lax.optimization_barrier((tuple(first), tuple(second)))


def odd_pairs(axis):
    size = lax.axis_size(axis)
    pairs = [(i, (i + 1) % size) for i in range(1, size, 2)]
    return pairs + [(j, i) for i, j in pairs]


def pair_exchange(near, far, axis):
    return (
        lax.ppermute(near, axis, flip(axis, 1)),
        lax.ppermute(far, axis, odd_pairs(axis)),
    )


def reduce_all(value, near_s, far_s, near_c, far_c):
    stream, cross = (lax.axis_size("stream"), lax.axis_size("cross"))
    half, quarter = (half_of("stream"), quarter_of("stream"))
    parts, back_a = together(
        scatter_sum(value, "stream", (1,), half),
        (lax.ppermute(near_s, "stream", flip("stream", 1)),),
    )
    value = pair_sum(parts)
    parts, back_c = together(
        scatter_sum(value, "stream", QUAD, quarter), pair_exchange(near_c, far_c, "cross")
    )
    value = pair_sum(parts)
    low = 8
    while low < stream:
        value = pair_sum(exchange(value, "stream", [low]))
        low *= 2
    parts, back_b = together(
        exchange(value, "cross", [1, 2]),
        (lax.ppermute(far_s, "stream", odd_pairs("stream")),),
    )
    value = pair_sum(parts)
    low = 4
    while low < cross:
        value = pair_sum(exchange(value, "cross", [low, 2 * low] if 2 * low < cross else [low]))
        low *= 4
    value = gather_back(value, "stream", QUAD, quarter)
    return (value, back_a + back_b + back_c)


def per_device(
    latents,
    stale_latents,
    edge_latents,
    senders,
    receivers,
    edge_count,
    send_list,
    node_cotangent,
    edge_cotangent,
    edge_first,
    edge_bias,
    edge_second,
    edge_gain,
    node_first,
    node_bias,
    node_second,
    node_gain,
):
    n, w = latents.shape
    e = edge_latents.shape[0]
    depth = send_list.shape[2]
    lists = send_list[0]

    sources = (
        latents,
        edge_latents,
        senders.reshape(e // w, w),
        receivers.reshape(e // w, w),
        node_cotangent,
        edge_cotangent,
        edge_first,
        edge_bias.reshape(1, w),
        edge_second,
        edge_gain.reshape(1, w),
        node_first,
        node_bias.reshape(1, w),
        node_second,
        node_gain.reshape(1, w),
    )
    loaded = call(
        load_kernel,
        (jax.ShapeDtypeStruct((depth, w), BF),) * 4
        + tuple(jax.ShapeDtypeStruct(x.shape, x.dtype) for x in sources),
        scratch=(
            pltpu.VMEM(lists.shape, lists.dtype),
            pltpu.VMEM((n, w), BF),
            pltpu.SemaphoreType.DMA((2 + len(sources),)),
        ),
        specs=[HB] * (2 + len(sources)),
        name="load",
    )(*(pltpu.with_memory_space_constraint(x, pltpu.HBM) for x in (lists, stale_latents) + sources))
    picked, kept = (loaded[:4], loaded[4:])
    halo = pair_exchange(picked[2], picked[3], "cross")
    halo = pair_exchange(picked[0], picked[1], "stream") + halo
    table = n + 4 * depth

    def shape(rows, kind=BF):
        return jax.ShapeDtypeStruct((rows, w), kind)

    new_latents, latent_grads, edge_grads, g0, g1, g2, g3, packed = call(
        main_kernel,
        (shape(n), shape(n), shape(e)) + (shape(depth),) * 4 + (shape(8 * w),),
        scratch=(
            pltpu.VMEM((table, w), BF),
            pltpu.VMEM((e, n), BF),
            pltpu.VMEM((n, e), BF),
            pltpu.VMEM((table, e), BF),
            pltpu.VMEM((e, w), BF),
            pltpu.VMEM((e, w), BF),
            pltpu.VMEM((e, w), BF),
            pltpu.VMEM((e, w), F32),
            pltpu.VMEM((e, w), F32),
            pltpu.VMEM((e, w), F32),
            pltpu.VMEM((e, w), BF),
            pltpu.VMEM((e, w), BF),
            pltpu.VMEM((e, w), BF),
        ),
        specs=[SM] + [VM] * 18,
        name="layer",
    )(
        edge_count, kept[0], *halo, *kept[1:]
    )
    part, returned = reduce_all(packed, g0, g1, g2, g3)
    stale_grads = call(stale_kernel, shape(n), specs=[VM] * 5, name="stale")(lists, *returned)
    other = lax.ppermute(part, "stream", flip("stream", 1))
    sizes = (3 * w * w, w, w * w, w, 2 * w * w, w, w * w, w)
    limit = math.sqrt(sum(sizes))
    clipped = call(
        functools.partial(final_kernel, limit),
        tuple(shape(s // w, F32) for s in sizes),
        specs=[VM, VM],
        name="clip",
    )(part, other)
    clipped = tuple(c.reshape(w) if s == w else c for c, s in zip(clipped, sizes))
    return (new_latents, latent_grads, stale_grads, edge_grads) + clipped


def solution(mesh):
    shard = P(("stream", "cross"))
    rows = P(("stream", "cross"), None)
    in_specs = (rows, rows, rows, shard, shard, shard, P(("stream", "cross"), None, None), rows, rows)
    in_specs = in_specs + (P(),) * 8
    out_specs = (rows,) * 4 + (P(),) * 8
    return jax.shard_map(
        per_device, mesh=mesh, in_specs=in_specs, out_specs=out_specs, check_vma=False
    )
```

```python
import functools
import math

import jax
import jax.numpy as jnp
from jax import lax
from jax.experimental import pallas as pl
from jax.experimental.pallas import tpu as pltpu
from jax.sharding import PartitionSpec as P

EPSILON = 1e-05
BF = jnp.bfloat16
F32 = jnp.float32
VMEM_LIMIT = 40 * 1024 * 1024


def mm(a, b):
    return jnp.dot(a, b, preferred_element_type=F32)


def mm_nt(a, b):
    return lax.dot_general(a, b, (((1,), (1,)), ((), ())), preferred_element_type=F32)


def mm_tn(a, b):
    return lax.dot_general(a, b, (((0,), (0,)), ((), ())), preferred_element_type=F32)


def index_columns(index_ref, row):
    line = index_ref[pl.ds(row, 1), :].astype(F32)
    return jnp.broadcast_to(line, (line.shape[1], line.shape[1])).T


def one_hot_rows(column, size):
    lanes = column.shape[1]
    lane = lax.broadcasted_iota(jnp.int32, column.shape, 1).astype(F32)
    blocks = [
        jnp.where(column == lane + float(base), 1.0, 0.0).astype(BF)
        for base in range(0, size, lanes)
    ]
    return jnp.concatenate(blocks, axis=1)


def one_hot_columns(index_ref, row, size, fold=False):
    line = index_ref[pl.ds(row, 1), :]
    if fold:
        line = jnp.where(line >= size, line - size, line)
    place = lax.broadcasted_iota(jnp.int32, (size, line.shape[1]), 0)
    return jnp.where(place == line, 1.0, 0.0).astype(BF)


def folded(column, half):
    upper = column >= float(half)
    return jnp.where(upper, column - float(half), column), upper


def side_by_side(rows):
    half = rows.shape[0] // 2
    return jnp.concatenate([rows[:half], rows[half:]], axis=1)


def stacked(pair):
    width = pair.shape[1] // 2
    return jnp.concatenate([pair[:, :width], pair[:, width:]], axis=0)


def chosen(pair, upper):
    width = pair.shape[1] // 2
    return jnp.where(upper, pair[:, width:], pair[:, :width])


def parted(rows, upper):
    zero = jnp.zeros_like(rows)
    return jnp.concatenate([jnp.where(upper, zero, rows), jnp.where(upper, rows, zero)], axis=1)


def parities():
    return (lax.rem(lax.axis_index("stream"), 2), lax.rem(lax.axis_index("cross"), 2))


def inner(axis):
    place = lax.axis_index(axis)
    return jnp.logical_and(place > 0, place < lax.axis_size(axis) - 1)


def list_order():
    odd_s, odd_c = parities()
    return (odd_s, 1 - odd_s, 2 + odd_c, 3 - odd_c)


def load_kernel(list_hbm, stale_hbm, *rest):
    count = (len(rest) - 5 - 2) // 2
    sources = rest[:count]
    outs = rest[count : count + 4]
    lists = rest[count + 4]
    kept = rest[count + 5 : 2 * count + 5]
    stale, sems = rest[2 * count + 5 :]
    copies = [
        pltpu.make_async_copy(a, b, sems.at[i])
        for i, (a, b) in enumerate(
            zip((list_hbm, stale_hbm) + sources, (lists, stale) + kept)
        )
    ]
    for copy in copies:
        copy.start()
    copies[0].wait()
    columns = [index_columns(lists, row) for row in list_order()]
    copies[1].wait()
    for column, out in zip(columns, outs):
        out[...] = mm(one_hot_rows(column, stale.shape[0]), stale[...]).astype(BF)
    for copy in copies[2:]:
        copy.wait()


def stale_kernel(list_ref, b0, b1, b2, b3, out_ref):
    total = None
    keep = (None, inner("stream"), None, inner("cross"))
    for row, part, valid in zip(list_order(), (b0, b1, b2, b3), keep):
        hot = one_hot_columns(list_ref, row, out_ref.shape[0])
        part = part[...]
        if valid is not None:
            part = jnp.where(valid, part, jnp.zeros_like(part))
        piece = mm(hot, part)
        total = piece if total is None else total + piece
    out_ref[...] = total.astype(BF)


def norm_forward(z):
    mean = jnp.mean(z, axis=-1, keepdims=True)
    centered = z - mean
    variance = jnp.mean(centered * centered, axis=-1, keepdims=True)
    inverse = lax.rsqrt(variance + EPSILON)
    return centered * inverse, jnp.broadcast_to(inverse, z.shape)


def norm_backward(slope, unit, inverse):
    first = jnp.mean(slope, axis=-1, keepdims=True)
    second = jnp.mean(slope * unit, axis=-1, keepdims=True)
    return inverse * (slope - first - unit * second)


def silu_pair(v):
    sig = 1.0 / (1.0 + jnp.exp(-v))
    hidden = v * sig
    return hidden, sig + hidden * (1.0 - sig)


def main_kernel(
    count_ref,
    latents,
    h0,
    h1,
    h2,
    h3,
    edges,
    senders,
    receivers,
    node_cot,
    edge_cot,
    edge_first,
    edge_bias,
    edge_second,
    edge_gain,
    node_first,
    node_bias,
    node_second,
    node_gain,
    new_latents,
    latent_grads,
    edge_grads,
    g0,
    g1,
    g2,
    g3,
    packed,
    table,
    hot_recv,
    turn_recv,
    turn_send,
    joined,
    hidden_s,
    slope_s,
    unit_s,
    inverse_s,
    upper_send,
    upper_recv,
    alive_edges,
    dz_s,
    dpre_s,
    dpre_send,
    dpre_recv,
    latent_out,
    grad_out,
    edge_out,
    sems,
):
    n, w = latents.shape
    e = edges.shape[0]
    t = table.shape[0]
    depth = h0.shape[0]
    chunk = 2 * w
    total = count_ref[0]
    table[:n] = latents[...]
    odd_s, odd_c = parities()
    for i, (near, far, odd, axis) in enumerate(
        ((h0, h1, odd_s, "stream"), (h2, h3, odd_c, "cross"))
    ):
        place = lax.axis_index(axis)
        a, b = (near[...], far[...])
        zero = jnp.zeros_like(a)
        before = jnp.where(place > 0, jnp.where(odd == 1, a, b), zero)
        after = jnp.where(place < lax.axis_size(axis) - 1, jnp.where(odd == 1, b, a), zero)
        at = n + 2 * i * depth
        table[at : at + depth] = before
        table[at + depth : at + 2 * depth] = after
    gain = edge_gain[...]

    for c in range(e // chunk):
        rows = slice(c * chunk, (c + 1) * chunk)
        for b in range(chunk // w):
            row = c * (chunk // w) + b
            part = slice(row * w, (row + 1) * w)
            column, upper = folded(index_columns(senders, row), t // 2)
            found = mm(one_hot_rows(column, t // 2), side_by_side(table))
            joined[part, :w] = chosen(found, upper).astype(BF)
            upper_send[part] = jnp.where(upper, 1.0, 0.0).astype(BF)
            column, upper = folded(index_columns(receivers, row), n // 2)
            hot = one_hot_rows(column, n // 2)
            hot_recv[part] = hot
            found = mm(hot, side_by_side(latents))
            joined[part, w:] = chosen(found, upper).astype(BF)
            upper_recv[part] = jnp.where(upper, 1.0, 0.0).astype(BF)
            turn_send[:, part] = one_hot_columns(senders, row, t // 2, True)
            turn_recv[:, part] = one_hot_columns(receivers, row, n // 2, True)
        edge = edges[rows]
        pre = mm(edge, edge_first[:w]) + mm(joined[rows], edge_first[w:]) + edge_bias[...]
        hidden, slope = silu_pair(pre)
        hidden = hidden.astype(BF)
        hidden_s[rows] = hidden
        slope_s[rows] = slope
        unit, inverse = norm_forward(mm(hidden, edge_second[...]))
        unit_s[rows] = unit
        inverse_s[rows] = inverse
        place = lax.broadcasted_iota(jnp.int32, (chunk, w), 0) + c * chunk
        fresh = (edge.astype(F32) + unit * gain).astype(BF)
        fresh = jnp.where(place < total, fresh, jnp.zeros_like(fresh))
        alive_edges[rows] = parted(fresh, upper_recv[rows] > 0)

    aggregate = stacked(mm(turn_recv[...], alive_edges[...])).astype(BF)
    own = latents[...]
    hidden, slope = silu_pair(
        mm(jnp.concatenate([own, aggregate], axis=1), node_first[...]) + node_bias[...]
    )
    hidden = hidden.astype(BF)
    unit, inverse = norm_forward(mm(hidden, node_second[...]))
    latent_out[...] = (own.astype(F32) + unit * node_gain[...]).astype(BF)
    send_latents = pltpu.make_async_copy(latent_out, new_latents, sems.at[0])
    send_latents.start()
    ncot = node_cot[...].astype(F32)
    node_gain_grad = jnp.sum(ncot * unit, axis=0, keepdims=True)
    dz = norm_backward(ncot * node_gain[...], unit, inverse).astype(BF)
    dpre = mm_nt(dz, node_second[...]) * slope
    node_bias_grad = jnp.sum(dpre, axis=0, keepdims=True)
    dpre = dpre.astype(BF)
    down = mm_nt(dpre, node_first[...])
    d_aggregate = side_by_side(down[:, w:].astype(BF))
    latent_part = ncot + down[:, :w]
    at = 4 * w
    packed[at : at + w] = mm_tn(own, dpre).astype(BF)
    packed[at + w : at + 2 * w] = mm_tn(aggregate, dpre).astype(BF)
    packed[at + 2 * w : at + 3 * w] = mm_tn(hidden, dz).astype(BF)

    bias_grad = jnp.zeros((1, w), F32)
    gain_grad = jnp.zeros((1, w), F32)
    for c in range(e // chunk):
        rows = slice(c * chunk, (c + 1) * chunk)
        place = lax.broadcasted_iota(jnp.int32, (chunk, w), 0) + c * chunk
        alive = place < total
        upper = upper_recv[rows] > 0
        passed = chosen(mm(hot_recv[rows], d_aggregate), upper)
        cot = edge_cot[rows].astype(F32) + jnp.where(alive, passed, 0.0)
        live = jnp.where(alive, cot, 0.0)
        unit = unit_s[rows]
        gain_grad = gain_grad + jnp.sum(live * unit, axis=0, keepdims=True)
        dz = norm_backward(live * gain, unit, inverse_s[rows]).astype(BF)
        dz_s[rows] = dz
        dpre = mm_nt(dz, edge_second[...]) * slope_s[rows]
        bias_grad = bias_grad + jnp.sum(dpre, axis=0, keepdims=True)
        dpre = dpre.astype(BF)
        dpre_s[rows] = dpre
        dpre_send[rows] = parted(dpre, upper_send[rows] > 0)
        dpre_recv[rows] = parted(dpre, upper)
        edge_out[rows] = (cot + mm_nt(dpre, edge_first[:w])).astype(BF)
    send_edges = pltpu.make_async_copy(edge_out, edge_grads, sems.at[1])
    send_edges.start()

    from_send = stacked(mm(turn_send[...], dpre_send[...])).astype(BF)
    from_recv = stacked(mm(turn_recv[...], dpre_recv[...])).astype(BF)
    back = mm_nt(from_send, edge_first[w : 2 * w])
    grad_out[...] = (latent_part + back[:n] + mm_nt(from_recv, edge_first[2 * w :])).astype(BF)
    send_grads = pltpu.make_async_copy(grad_out, latent_grads, sems.at[2])
    send_grads.start()
    for i, (near, far, odd) in enumerate(((g0, g1, odd_s), (g2, g3, odd_c))):
        at = n + 2 * i * depth
        before = back[at : at + depth]
        after = back[at + depth : at + 2 * depth]
        near[...] = jnp.where(odd == 1, before, after).astype(BF)
        far[...] = jnp.where(odd == 1, after, before).astype(BF)

    dpre = dpre_s[...]
    packed[:w] = mm_tn(edges[...], dpre).astype(BF)
    packed[w : 3 * w] = mm_tn(joined[...], dpre).astype(BF)
    packed[3 * w : 4 * w] = mm_tn(hidden_s[...], dz_s[...]).astype(BF)
    tail = jnp.concatenate(
        [bias_grad, gain_grad, node_bias_grad, node_gain_grad, jnp.zeros((w - 4, w), F32)], axis=0
    )
    packed[7 * w :] = tail.astype(BF)
    send_latents.wait()
    send_edges.wait()
    send_grads.wait()


def final_kernel(limit, mine, other, *outs):
    swap = half_of("stream") == 1
    a, b = (mine[...].astype(F32), other[...].astype(F32))
    low = jnp.where(swap, b, a)
    high = jnp.where(swap, a, b)
    squares = jnp.sum(a * a + b * b)
    factor = jnp.minimum(1.0, limit * lax.rsqrt(jnp.full((1, a.shape[1]), squares, F32)))
    w = a.shape[1]
    full = (low * factor, high * factor)
    ef, eb, es, eg, nf, nb, ns, ng = outs
    half = 4 * w
    ef[...] = full[0][: 3 * w]
    es[...] = full[0][3 * w :]
    nf[...] = full[1][: 2 * w]
    ns[...] = full[1][2 * w : 3 * w]
    eb[...] = full[1][3 * w : 3 * w + 1]
    eg[...] = full[1][3 * w + 1 : 3 * w + 2]
    nb[...] = full[1][3 * w + 2 : 3 * w + 3]
    ng[...] = full[1][3 * w + 3 : 3 * w + 4]


VM = pl.BlockSpec(memory_space=pltpu.VMEM)
SM = pl.BlockSpec(memory_space=pltpu.SMEM)
HB = pl.BlockSpec(memory_space=pltpu.HBM)


def call(kernel, outs, scratch=(), specs=None, name=None, out_specs=None):
    return pl.pallas_call(
        kernel,
        out_shape=outs,
        in_specs=specs,
        out_specs=out_specs or jax.tree.map(lambda _: VM, outs),
        scratch_shapes=list(scratch),
        compiler_params=pltpu.CompilerParams(vmem_limit_bytes=VMEM_LIMIT),
        name=name,
    )


def flip(axis, bit):
    return [(i, i ^ bit) for i in range(lax.axis_size(axis))]


def pair_sum(parts):
    parts = [p.astype(F32) for p in parts]
    while len(parts) > 1:
        parts = [parts[i] + parts[i + 1] for i in range(0, len(parts), 2)]
    return parts[0].astype(BF)


def exchange(value, axis, bits):
    out = [value]
    for m in range(1, 1 << len(bits)):
        mask = sum(bits[j] for j in range(len(bits)) if m >> j & 1)
        out.append(lax.ppermute(value, axis, flip(axis, mask)))
    return out


def scatter_sum(value, axis, masks, spot):
    radix = len(masks) + 1
    blocks = value.reshape((radix, value.shape[0] // radix) + value.shape[1:])
    got = [lax.dynamic_index_in_dim(blocks, spot, 0, False)]
    for k, mask in enumerate(masks):
        block = lax.dynamic_index_in_dim(blocks, spot ^ (k + 1), 0, False)
        got.append(lax.ppermute(block, axis, flip(axis, mask)))
    return got


def gather_back(value, axis, masks, spot):
    stack = jnp.stack([value] + [lax.ppermute(value, axis, flip(axis, m)) for m in masks])
    return jnp.concatenate(
        [lax.dynamic_index_in_dim(stack, spot ^ k, 0, False) for k in range(len(masks) + 1)],
        axis=0,
    )


QUAD = (3, 4, 7)


def half_of(axis):
    place = lax.axis_index(axis)
    return lax.rem(place, 2) ^ lax.rem(place // 2, 2)


def quarter_of(axis):
    return lax.rem(lax.axis_index(axis) // 2, 4)


def together(first, *rest):
    return lax.optimization_barrier((first,) + rest)


def odd_exchange(value, axis):
    stream, cross = (lax.axis_size("stream"), lax.axis_size("cross"))
    pairs = []
    for s in range(stream):
        for c in range(cross):
            place, size = (s, stream) if axis == "stream" else (c, cross)
            to = place + 1 if place % 2 else place - 1
            if axis == "stream":
                peer = (to, c) if 0 <= to < size else (s, c ^ 1)
            else:
                peer = (s, to) if 0 <= to < size else (s ^ 1, c)
            pairs.append((s * cross + c, peer[0] * cross + peer[1]))
    return lax.ppermute(value, ("stream", "cross"), pairs)


def pair_exchange(near, far, axis):
    return (lax.ppermute(near, axis, flip(axis, 1)), odd_exchange(far, axis))


def reduce_all(value, near_s, far_s, near_c, far_c):
    stream, cross = (lax.axis_size("stream"), lax.axis_size("cross"))
    half, quarter = (half_of("stream"), quarter_of("stream"))
    depth = near_s.shape[0]
    blocks = value.reshape((2, value.shape[0] // 2, value.shape[1]))
    mine = lax.dynamic_index_in_dim(blocks, half, 0, False)
    give = lax.dynamic_index_in_dim(blocks, 1 - half, 0, False)
    back_c = lax.ppermute(near_c, "cross", flip("cross", 1))
    got = lax.ppermute(jnp.concatenate([give, near_s]), "stream", flip("stream", 1))
    value = pair_sum([mine, got[: mine.shape[0]]])
    back_s = got[mine.shape[0] :]
    value, far_c = together(value, far_c)
    back_d = odd_exchange(far_c, "cross")
    parts, back_c = together(scatter_sum(value, "stream", QUAD, quarter), back_c)
    value = pair_sum(parts)
    low = 8
    while low < stream:
        value = pair_sum(exchange(value, "stream", [low]))
        low *= 2
    value, far_s = together(value, far_s)
    back_b = odd_exchange(far_s, "stream")
    parts, back_d, back_b = together(exchange(value, "cross", [1, 2]), back_d, back_b)
    value = pair_sum(parts)
    low = 4
    while low < cross:
        value = pair_sum(exchange(value, "cross", [low, 2 * low] if 2 * low < cross else [low]))
        low *= 4
    value = gather_back(value, "stream", QUAD, quarter)
    return (value, (back_s, back_b, back_c, back_d))


def per_device(
    latents,
    stale_latents,
    edge_latents,
    senders,
    receivers,
    edge_count,
    send_list,
    node_cotangent,
    edge_cotangent,
    edge_first,
    edge_bias,
    edge_second,
    edge_gain,
    node_first,
    node_bias,
    node_second,
    node_gain,
):
    n, w = latents.shape
    e = edge_latents.shape[0]
    depth = send_list.shape[2]
    lists = send_list[0]

    sources = (
        latents,
        edge_latents,
        senders.reshape(e // w, w),
        receivers.reshape(e // w, w),
        node_cotangent,
        edge_cotangent,
        edge_first,
        edge_bias.reshape(1, w),
        edge_second,
        edge_gain.reshape(1, w),
        node_first,
        node_bias.reshape(1, w),
        node_second,
        node_gain.reshape(1, w),
    )
    loaded = call(
        load_kernel,
        (jax.ShapeDtypeStruct((depth, w), BF),) * 4
        + (jax.ShapeDtypeStruct(lists.shape, lists.dtype),)
        + tuple(jax.ShapeDtypeStruct(x.shape, x.dtype) for x in sources),
        scratch=(
            pltpu.VMEM((n, w), BF),
            pltpu.SemaphoreType.DMA((2 + len(sources),)),
        ),
        specs=[HB] * (2 + len(sources)),
        name="load",
    )(*(pltpu.with_memory_space_constraint(x, pltpu.HBM) for x in (lists, stale_latents) + sources))
    picked, lists, kept = (loaded[:4], loaded[4], loaded[5:])
    halo = pair_exchange(picked[2], picked[3], "cross")
    halo = pair_exchange(picked[0], picked[1], "stream") + halo
    table = n + 4 * depth

    def shape(rows, kind=BF):
        return jax.ShapeDtypeStruct((rows, w), kind)

    new_latents, latent_grads, edge_grads, g0, g1, g2, g3, packed = call(
        main_kernel,
        (shape(n), shape(n), shape(e)) + (shape(depth),) * 4 + (shape(8 * w),),
        scratch=(
            pltpu.VMEM((table, w), BF),
            pltpu.VMEM((e, n // 2), BF),
            pltpu.VMEM((n // 2, e), BF),
            pltpu.VMEM((table // 2, e), BF),
            pltpu.VMEM((e, 2 * w), BF),
            pltpu.VMEM((e, w), BF),
            pltpu.VMEM((e, w), F32),
            pltpu.VMEM((e, w), F32),
            pltpu.VMEM((e, w), F32),
            pltpu.VMEM((e, w), BF),
            pltpu.VMEM((e, w), BF),
            pltpu.VMEM((e, 2 * w), BF),
            pltpu.VMEM((e, w), BF),
            pltpu.VMEM((e, w), BF),
            pltpu.VMEM((e, 2 * w), BF),
            pltpu.VMEM((e, 2 * w), BF),
            pltpu.VMEM((n, w), BF),
            pltpu.VMEM((n, w), BF),
            pltpu.VMEM((e, w), BF),
            pltpu.SemaphoreType.DMA((3,)),
        ),
        specs=[SM] + [VM] * 18,
        out_specs=(HB,) * 3 + (VM,) * 5,
        name="layer",
    )(
        edge_count, kept[0], *halo, *kept[1:]
    )
    part, returned = reduce_all(packed, g0, g1, g2, g3)
    stale_grads = call(stale_kernel, shape(n), specs=[VM] * 5, name="stale")(lists, *returned)
    other = lax.ppermute(part, "stream", flip("stream", 1))
    sizes = (3 * w * w, w, w * w, w, 2 * w * w, w, w * w, w)
    limit = math.sqrt(sum(sizes))
    clipped = call(
        functools.partial(final_kernel, limit),
        tuple(shape(s // w, F32) for s in sizes),
        specs=[VM, VM],
        name="clip",
    )(part, other)
    clipped = tuple(c.reshape(w) if s == w else c for c, s in zip(clipped, sizes))
    return (new_latents, latent_grads, stale_grads, edge_grads) + clipped


def solution(mesh):
    shard = P(("stream", "cross"))
    rows = P(("stream", "cross"), None)
    in_specs = (rows, rows, rows, shard, shard, shard, P(("stream", "cross"), None, None), rows, rows)
    in_specs = in_specs + (P(),) * 8
    out_specs = (rows,) * 4 + (P(),) * 8
    return jax.shard_map(
        per_device, mesh=mesh, in_specs=in_specs, out_specs=out_specs, check_vma=False
    )
```

```python
import functools
import math

import jax
import jax.numpy as jnp
from jax import lax
from jax.experimental import pallas as pl
from jax.experimental.pallas import tpu as pltpu
from jax.sharding import PartitionSpec as P


EPSILON = 1e-05
BF = jnp.bfloat16
F32 = jnp.float32
VMEM_LIMIT = 40 * 1024 * 1024


def mm(a, b):
    return jnp.dot(a, b, preferred_element_type=F32)


def mm_nt(a, b):
    return lax.dot_general(a, b, (((1,), (1,)), ((), ())), preferred_element_type=F32)


def mm_tn(a, b):
    return lax.dot_general(a, b, (((0,), (0,)), ((), ())), preferred_element_type=F32)


def index_columns(index_ref, row):
    line = index_ref[pl.ds(row, 1), :].astype(F32)
    return jnp.broadcast_to(line, (line.shape[1], line.shape[1])).T


I16 = jnp.int16


def ones_where(mask, shape):
    return jnp.where(mask, jnp.ones(shape, BF), jnp.zeros(shape, BF))


def one_hot_rows(column, size):
    lanes = column.shape[1]
    lane = lax.broadcasted_iota(jnp.int32, column.shape, 1)
    short = column.astype(jnp.int32).astype(I16)
    blocks = [
        ones_where(short == (lane + base).astype(I16), column.shape)
        for base in range(0, size, lanes)
    ]
    return jnp.concatenate(blocks, axis=1)


def one_hot_columns(index_ref, row, size, fold=False):
    line = index_ref[pl.ds(row, 1), :]
    if fold:
        line = jnp.where(line >= size, line - size, line)
    shape = (size, line.shape[1])
    tile = jnp.broadcast_to(line, (16, line.shape[1])).astype(I16)
    place = lax.broadcasted_iota(jnp.int32, shape, 0).astype(I16)
    return ones_where(place == jnp.concatenate([tile] * (size // 16), axis=0), shape)


def folded(column, half):
    upper = column >= float(half)
    return jnp.where(upper, column - float(half), column), upper


def side_by_side(rows):
    half = rows.shape[0] // 2
    return jnp.concatenate([rows[:half], rows[half:]], axis=1)


def stacked(pair):
    width = pair.shape[1] // 2
    return jnp.concatenate([pair[:, :width], pair[:, width:]], axis=0)


def chosen(pair, upper):
    width = pair.shape[1] // 2
    return jnp.where(upper, pair[:, width:], pair[:, :width])


def parted(rows, upper):
    zero = jnp.zeros_like(rows)
    return jnp.concatenate([jnp.where(upper, zero, rows), jnp.where(upper, rows, zero)], axis=1)


def parities():
    return (lax.rem(lax.axis_index("stream"), 2), lax.rem(lax.axis_index("cross"), 2))


def inner(axis):
    place = lax.axis_index(axis)
    return jnp.logical_and(place > 0, place < lax.axis_size(axis) - 1)


def list_order():
    odd_s, odd_c = parities()
    return (odd_s, 1 - odd_s, 2 + odd_c, 3 - odd_c)


def load_kernel(list_hbm, stale_hbm, *rest):
    count = (len(rest) - 5 - 2) // 2
    sources = rest[:count]
    outs = rest[count : count + 4]
    lists = rest[count + 4]
    kept = rest[count + 5 : 2 * count + 5]
    stale, sems = rest[2 * count + 5 :]
    copies = [
        pltpu.make_async_copy(a, b, sems.at[i])
        for i, (a, b) in enumerate(
            zip((list_hbm, stale_hbm) + sources, (lists, stale) + kept)
        )
    ]
    for copy in copies:
        copy.start()
    copies[0].wait()
    columns = [index_columns(lists, row) for row in list_order()]
    copies[1].wait()
    for column, out in zip(columns, outs):
        out[...] = mm(one_hot_rows(column, stale.shape[0]), stale[...]).astype(BF)
    for copy in copies[2:]:
        copy.wait()


def stale_kernel(list_ref, b0, b1, b2, b3, out_ref):
    total = None
    keep = (None, inner("stream"), None, inner("cross"))
    for row, part, valid in zip(list_order(), (b0, b1, b2, b3), keep):
        hot = one_hot_columns(list_ref, row, out_ref.shape[0])
        part = part[...]
        if valid is not None:
            part = jnp.where(valid, part, jnp.zeros_like(part))
        piece = mm(hot, part)
        total = piece if total is None else total + piece
    out_ref[...] = total.astype(BF)


def norm_forward(z):
    mean = jnp.mean(z, axis=-1, keepdims=True)
    centered = z - mean
    variance = jnp.mean(centered * centered, axis=-1, keepdims=True)
    inverse = lax.rsqrt(variance + EPSILON)
    return centered * inverse, jnp.broadcast_to(inverse, z.shape)


def norm_backward(slope, unit, inverse):
    first = jnp.mean(slope, axis=-1, keepdims=True)
    second = jnp.mean(slope * unit, axis=-1, keepdims=True)
    return inverse * (slope - first - unit * second)


def silu_pair(v):
    sig = 0.5 * jnp.tanh(0.5 * v) + 0.5
    hidden = v * sig
    return hidden, sig + hidden * (1.0 - sig)


def main_kernel(
    count_ref,
    latents,
    h0,
    h1,
    h2,
    h3,
    edges,
    senders,
    receivers,
    node_cot,
    edge_cot,
    edge_first,
    edge_bias,
    edge_second,
    edge_gain,
    node_first,
    node_bias,
    node_second,
    node_gain,
    new_latents,
    latent_grads,
    edge_grads,
    g0,
    g1,
    g2,
    g3,
    packed,
    table,
    hot_recv,
    turn_recv,
    turn_send,
    joined,
    hidden_s,
    slope_s,
    unit_s,
    inverse_s,
    upper_send,
    upper_recv,
    alive_edges,
    dz_s,
    dpre_s,
    dpre_send,
    dpre_recv,
    latent_out,
    grad_out,
    edge_out,
    sems,
):
    n, w = latents.shape
    e = edges.shape[0]
    t = table.shape[0]
    depth = h0.shape[0]
    chunk = e // 2
    total = count_ref[0]
    table[:n] = latents[...]
    odd_s, odd_c = parities()
    for i, (near, far, odd, axis) in enumerate(
        ((h0, h1, odd_s, "stream"), (h2, h3, odd_c, "cross"))
    ):
        place = lax.axis_index(axis)
        a, b = (near[...], far[...])
        zero = jnp.zeros_like(a)
        before = jnp.where(place > 0, jnp.where(odd == 1, a, b), zero)
        after = jnp.where(place < lax.axis_size(axis) - 1, jnp.where(odd == 1, b, a), zero)
        at = n + 2 * i * depth
        table[at : at + depth] = before
        table[at + depth : at + 2 * depth] = after
    gain = edge_gain[...]

    for c in range(e // chunk):
        rows = slice(c * chunk, (c + 1) * chunk)
        for b in range(chunk // w):
            row = c * (chunk // w) + b
            part = slice(row * w, (row + 1) * w)
            column, upper = folded(index_columns(senders, row), t // 2)
            found = mm(one_hot_rows(column, t // 2), side_by_side(table))
            joined[part, :w] = chosen(found, upper).astype(BF)
            upper_send[part] = jnp.where(upper, 1.0, 0.0).astype(BF)
            column, upper = folded(index_columns(receivers, row), n // 2)
            hot = one_hot_rows(column, n // 2)
            hot_recv[part] = hot
            found = mm(hot, side_by_side(latents))
            joined[part, w:] = chosen(found, upper).astype(BF)
            upper_recv[part] = jnp.where(upper, 1.0, 0.0).astype(BF)
            turn_send[:, part] = one_hot_columns(senders, row, t // 2, True)
            turn_recv[:, part] = one_hot_columns(receivers, row, n // 2, True)
        edge = edges[rows]
        pre = mm(edge, edge_first[:w]) + mm(joined[rows], edge_first[w:]) + edge_bias[...]
        hidden, slope = silu_pair(pre)
        hidden = hidden.astype(BF)
        hidden_s[rows] = hidden
        slope_s[rows] = slope
        unit, inverse = norm_forward(mm(hidden, edge_second[...]))
        unit_s[rows] = unit
        inverse_s[rows] = inverse
        place = lax.broadcasted_iota(jnp.int32, (chunk, w), 0) + c * chunk
        fresh = (edge.astype(F32) + unit * gain).astype(BF)
        fresh = jnp.where(place < total, fresh, jnp.zeros_like(fresh))
        alive_edges[rows] = parted(fresh, upper_recv[rows] > 0)

    aggregate = stacked(mm(turn_recv[...], alive_edges[...])).astype(BF)
    own = latents[...]
    hidden, slope = silu_pair(
        mm(jnp.concatenate([own, aggregate], axis=1), node_first[...]) + node_bias[...]
    )
    hidden = hidden.astype(BF)
    unit, inverse = norm_forward(mm(hidden, node_second[...]))
    latent_out[...] = (own.astype(F32) + unit * node_gain[...]).astype(BF)
    send_latents = pltpu.make_async_copy(latent_out, new_latents, sems.at[0])
    send_latents.start()
    ncot = node_cot[...].astype(F32)
    node_gain_grad = jnp.sum(ncot * unit, axis=0, keepdims=True)
    dz = norm_backward(ncot * node_gain[...], unit, inverse).astype(BF)
    dpre = mm_nt(dz, node_second[...]) * slope
    node_bias_grad = jnp.sum(dpre, axis=0, keepdims=True)
    dpre = dpre.astype(BF)
    down = mm_nt(dpre, node_first[...])
    d_aggregate = side_by_side(down[:, w:].astype(BF))
    latent_part = ncot + down[:, :w]
    at = 4 * w
    packed[at : at + w] = mm_tn(own, dpre).astype(BF)
    packed[at + w : at + 2 * w] = mm_tn(aggregate, dpre).astype(BF)
    packed[at + 2 * w : at + 3 * w] = mm_tn(hidden, dz).astype(BF)

    bias_grad = jnp.zeros((1, w), F32)
    gain_grad = jnp.zeros((1, w), F32)
    for c in range(e // chunk):
        rows = slice(c * chunk, (c + 1) * chunk)
        place = lax.broadcasted_iota(jnp.int32, (chunk, w), 0) + c * chunk
        alive = place < total
        upper = upper_recv[rows] > 0
        passed = chosen(mm(hot_recv[rows], d_aggregate), upper)
        cot = edge_cot[rows].astype(F32) + jnp.where(alive, passed, 0.0)
        live = jnp.where(alive, cot, 0.0)
        unit = unit_s[rows]
        gain_grad = gain_grad + jnp.sum(live * unit, axis=0, keepdims=True)
        dz = norm_backward(live * gain, unit, inverse_s[rows]).astype(BF)
        dz_s[rows] = dz
        dpre = mm_nt(dz, edge_second[...]) * slope_s[rows]
        bias_grad = bias_grad + jnp.sum(dpre, axis=0, keepdims=True)
        dpre = dpre.astype(BF)
        dpre_s[rows] = dpre
        dpre_send[rows] = parted(dpre, upper_send[rows] > 0)
        dpre_recv[rows] = parted(dpre, upper)
        edge_out[rows] = (cot + mm_nt(dpre, edge_first[:w])).astype(BF)
    send_edges = pltpu.make_async_copy(edge_out, edge_grads, sems.at[1])
    send_edges.start()

    from_send = stacked(mm(turn_send[...], dpre_send[...])).astype(BF)
    from_recv = stacked(mm(turn_recv[...], dpre_recv[...])).astype(BF)
    back = mm_nt(from_send, edge_first[w : 2 * w])
    grad_out[...] = (latent_part + back[:n] + mm_nt(from_recv, edge_first[2 * w :])).astype(BF)
    send_grads = pltpu.make_async_copy(grad_out, latent_grads, sems.at[2])
    send_grads.start()
    for i, (near, far, odd) in enumerate(((g0, g1, odd_s), (g2, g3, odd_c))):
        at = n + 2 * i * depth
        before = back[at : at + depth]
        after = back[at + depth : at + 2 * depth]
        near[...] = jnp.where(odd == 1, before, after).astype(BF)
        far[...] = jnp.where(odd == 1, after, before).astype(BF)

    dpre = dpre_s[...]
    packed[:w] = mm_tn(edges[...], dpre).astype(BF)
    packed[w : 3 * w] = mm_tn(joined[...], dpre).astype(BF)
    packed[3 * w : 4 * w] = mm_tn(hidden_s[...], dz_s[...]).astype(BF)
    tail = jnp.concatenate(
        [
            bias_grad,
            gain_grad,
            node_bias_grad,
            node_gain_grad,
            jnp.zeros((packed.shape[0] - 7 * w - 4, w), F32),
        ],
        axis=0,
    )
    packed[7 * w :] = tail.astype(BF)
    send_latents.wait()
    send_edges.wait()
    send_grads.wait()


def final_kernel(limit, mine, other, *outs):
    swap = half_of() == 1
    a, b = (mine[...].astype(F32), other[...].astype(F32))
    low = jnp.where(swap, b, a)
    high = jnp.where(swap, a, b)
    squares = jnp.sum(a * a + b * b)
    factor = jnp.minimum(1.0, limit * lax.rsqrt(jnp.full((1, a.shape[1]), squares, F32)))
    full = jnp.concatenate([low, high], axis=0) * factor
    ef, eb, es, eg, nf, nb, ns, ng = outs
    at = 0
    for out in (ef, es, nf, ns, eb, eg, nb, ng):
        out[...] = full[at : at + out.shape[0]]
        at += out.shape[0]


VM = pl.BlockSpec(memory_space=pltpu.VMEM)
SM = pl.BlockSpec(memory_space=pltpu.SMEM)
HB = pl.BlockSpec(memory_space=pltpu.HBM)


def call(kernel, outs, scratch=(), specs=None, out_specs=None):
    return pl.pallas_call(
        kernel,
        out_shape=outs,
        in_specs=specs,
        out_specs=out_specs or jax.tree.map(lambda _: VM, outs),
        scratch_shapes=list(scratch),
        compiler_params=pltpu.CompilerParams(vmem_limit_bytes=VMEM_LIMIT),
    )


def flip(axis, bit):
    return [(i, i ^ bit) for i in range(lax.axis_size(axis))]


def pair_sum(parts):
    parts = [p.astype(F32) for p in parts]
    while len(parts) > 1:
        parts = [parts[i] + parts[i + 1] for i in range(0, len(parts), 2)]
    return parts[0].astype(BF)


def level_flip(mask):
    stream, cross = (lax.axis_size("stream"), lax.axis_size("cross"))
    turn = mask >> 1 & 1
    return [
        (s * cross + c, (s ^ turn) * cross + (c ^ mask)) for s in range(stream) for c in range(cross)
    ]


def level_exchange(value, bits):
    out = [value]
    for m in range(1, 1 << len(bits)):
        mask = sum(bits[j] for j in range(len(bits)) if m >> j & 1)
        out.append(lax.ppermute(value, ("stream", "cross"), level_flip(mask)))
    return out


def exchange(value, axis, bits):
    out = [value]
    for m in range(1, 1 << len(bits)):
        mask = sum(bits[j] for j in range(len(bits)) if m >> j & 1)
        out.append(lax.ppermute(value, axis, flip(axis, mask)))
    return out


def scatter_sum(value, axis, masks, spot):
    radix = len(masks) + 1
    blocks = value.reshape((radix, value.shape[0] // radix) + value.shape[1:])
    got = [lax.dynamic_index_in_dim(blocks, spot, 0, False)]
    for k, mask in enumerate(masks):
        block = lax.dynamic_index_in_dim(blocks, spot ^ (k + 1), 0, False)
        got.append(lax.ppermute(block, axis, flip(axis, mask)))
    return got


def gather_back(value, axis, masks, spot):
    stack = jnp.stack([value] + [lax.ppermute(value, axis, flip(axis, m)) for m in masks])
    return jnp.concatenate(
        [lax.dynamic_index_in_dim(stack, spot ^ k, 0, False) for k in range(len(masks) + 1)],
        axis=0,
    )


QUAD = (3, 4, 7)


def half_of():
    place, level = (lax.axis_index("stream"), lax.axis_index("cross"))
    return lax.rem(place, 2) ^ lax.rem(place // 2, 2) ^ lax.rem(level // 2, 2)


def quarter_of(axis):
    return lax.rem(lax.axis_index(axis) // 2, 4)


def together(first, *rest):
    return lax.optimization_barrier((first,) + rest)


def odd_exchange(value, axis):
    stream, cross = (lax.axis_size("stream"), lax.axis_size("cross"))
    pairs = []
    for s in range(stream):
        for c in range(cross):
            place, size = (s, stream) if axis == "stream" else (c, cross)
            to = place + 1 if place % 2 else place - 1
            if axis == "stream":
                peer = (to, c) if 0 <= to < size else (s, c ^ 1)
            else:
                peer = (s, to) if 0 <= to < size else (s ^ 1, c)
            pairs.append((s * cross + c, peer[0] * cross + peer[1]))
    return lax.ppermute(value, ("stream", "cross"), pairs)


def pair_exchange(near, far, axis):
    return (lax.ppermute(near, axis, flip(axis, 1)), odd_exchange(far, axis))


def reduce_all(value, near_s, far_s, near_c, far_c):
    stream, cross = (lax.axis_size("stream"), lax.axis_size("cross"))
    half, quarter = (half_of(), quarter_of("stream"))
    blocks = value.reshape((2, value.shape[0] // 2, value.shape[1]))
    mine = lax.dynamic_index_in_dim(blocks, half, 0, False)
    give = lax.dynamic_index_in_dim(blocks, 1 - half, 0, False)
    back_c = lax.ppermute(near_c, "cross", flip("cross", 1))
    got = lax.ppermute(jnp.concatenate([give, near_s]), "stream", flip("stream", 1))
    value = pair_sum([mine, got[: mine.shape[0]]])
    back_s = got[mine.shape[0] :]
    value, far_c = together(value, far_c)
    back_d = odd_exchange(far_c, "cross")
    parts, back_c = together(scatter_sum(value, "stream", QUAD, quarter), back_c)
    value = pair_sum(parts)
    low = 8
    while low < stream:
        value = pair_sum(exchange(value, "stream", [low]))
        low *= 2
    value, far_s = together(value, far_s)
    parts = level_exchange(value, [1, 2])
    back_b = odd_exchange(far_s, "stream")
    parts, back_d, back_b = together(parts, back_d, back_b)
    value = pair_sum(parts)
    low = 4
    while low < cross:
        value = pair_sum(level_exchange(value, [low, 2 * low] if 2 * low < cross else [low]))
        low *= 4
    value = gather_back(value, "stream", QUAD, quarter)
    return (value, (back_s, back_b, back_c, back_d))


def per_device(
    latents,
    stale_latents,
    edge_latents,
    senders,
    receivers,
    edge_count,
    send_list,
    node_cotangent,
    edge_cotangent,
    edge_first,
    edge_bias,
    edge_second,
    edge_gain,
    node_first,
    node_bias,
    node_second,
    node_gain,
):
    n, w = latents.shape
    e = edge_latents.shape[0]
    depth = send_list.shape[2]
    lists = send_list[0]

    sources = (
        latents,
        edge_latents,
        senders.reshape(e // w, w),
        receivers.reshape(e // w, w),
        node_cotangent,
        edge_cotangent,
        edge_first,
        edge_bias.reshape(1, w),
        edge_second,
        edge_gain.reshape(1, w),
        node_first,
        node_bias.reshape(1, w),
        node_second,
        node_gain.reshape(1, w),
    )
    loaded = call(
        load_kernel,
        (jax.ShapeDtypeStruct((depth, w), BF),) * 4
        + (jax.ShapeDtypeStruct(lists.shape, lists.dtype),)
        + tuple(jax.ShapeDtypeStruct(x.shape, x.dtype) for x in sources),
        scratch=(
            pltpu.VMEM((n, w), BF),
            pltpu.SemaphoreType.DMA((2 + len(sources),)),
        ),
        specs=[HB] * (2 + len(sources)),
    )(*(pltpu.with_memory_space_constraint(x, pltpu.HBM) for x in (lists, stale_latents) + sources))
    picked, lists, kept = (loaded[:4], loaded[4], loaded[5:])
    halo = pair_exchange(picked[2], picked[3], "cross")
    halo = pair_exchange(picked[0], picked[1], "stream") + halo
    table = n + 4 * depth

    def shape(rows, kind=BF):
        return jax.ShapeDtypeStruct((rows, w), kind)

    new_latents, latent_grads, edge_grads, g0, g1, g2, g3, packed = call(
        main_kernel,
        (shape(n), shape(n), shape(e)) + (shape(depth),) * 4 + (shape(-(-(7 * w + 4) // 64) * 64),),
        scratch=(
            pltpu.VMEM((table, w), BF),
            pltpu.VMEM((e, n // 2), BF),
            pltpu.VMEM((n // 2, e), BF),
            pltpu.VMEM((table // 2, e), BF),
            pltpu.VMEM((e, 2 * w), BF),
            pltpu.VMEM((e, w), BF),
            pltpu.VMEM((e, w), F32),
            pltpu.VMEM((e, w), F32),
            pltpu.VMEM((e, w), F32),
            pltpu.VMEM((e, w), BF),
            pltpu.VMEM((e, w), BF),
            pltpu.VMEM((e, 2 * w), BF),
            pltpu.VMEM((e, w), BF),
            pltpu.VMEM((e, w), BF),
            pltpu.VMEM((e, 2 * w), BF),
            pltpu.VMEM((e, 2 * w), BF),
            pltpu.VMEM((n, w), BF),
            pltpu.VMEM((n, w), BF),
            pltpu.VMEM((e, w), BF),
            pltpu.SemaphoreType.DMA((3,)),
        ),
        specs=[SM] + [VM] * 18,
        out_specs=(HB,) * 3 + (VM,) * 5,
    )(
        edge_count, kept[0], *halo, *kept[1:]
    )
    part, returned = reduce_all(packed, g0, g1, g2, g3)
    stale_grads = call(stale_kernel, shape(n), specs=[VM] * 5)(lists, *returned)
    other = lax.ppermute(part, "stream", flip("stream", 1))
    sizes = (3 * w * w, w, w * w, w, 2 * w * w, w, w * w, w)
    limit = math.sqrt(sum(sizes))
    clipped = call(
        functools.partial(final_kernel, limit),
        tuple(shape(s // w, F32) for s in sizes),
        specs=[VM, VM],
    )(part, other)
    clipped = tuple(c.reshape(w) if s == w else c for c, s in zip(clipped, sizes))
    return (new_latents, latent_grads, stale_grads, edge_grads) + clipped


def solution(mesh):
    shard = P(("stream", "cross"))
    rows = P(("stream", "cross"), None)
    in_specs = (rows, rows, rows, shard, shard, shard, P(("stream", "cross"), None, None), rows, rows)
    in_specs = in_specs + (P(),) * 8
    out_specs = (rows,) * 4 + (P(),) * 8
    return jax.shard_map(
        per_device, mesh=mesh, in_specs=in_specs, out_specs=out_specs, check_vma=False
    )
```

```python
import functools
import math

import jax
import jax.numpy as jnp
from jax import lax
from jax.experimental import pallas as pl
from jax.experimental.pallas import tpu as pltpu
from jax.sharding import PartitionSpec as P


EPSILON = 1e-05
BF = jnp.bfloat16
F32 = jnp.float32
VMEM_LIMIT = 40 * 1024 * 1024


def mm(a, b):
    return jnp.dot(a, b, preferred_element_type=F32)


def mm_nt(a, b):
    return lax.dot_general(a, b, (((1,), (1,)), ((), ())), preferred_element_type=F32)


def mm_tn(a, b):
    return lax.dot_general(a, b, (((0,), (0,)), ((), ())), preferred_element_type=F32)


def index_columns(index_ref, row):
    line = index_ref[pl.ds(row, 1), :].astype(F32)
    return jnp.broadcast_to(line, (line.shape[1], line.shape[1])).T


I16 = jnp.int16


def ones_where(mask, shape):
    return jnp.where(mask, jnp.ones(shape, BF), jnp.zeros(shape, BF))


def one_hot_rows(column, size):
    lanes = column.shape[1]
    lane = lax.broadcasted_iota(jnp.int32, column.shape, 1)
    short = column.astype(jnp.int32).astype(I16)
    blocks = [
        ones_where(short == (lane + base).astype(I16), column.shape)
        for base in range(0, size, lanes)
    ]
    return jnp.concatenate(blocks, axis=1)


def one_hot_columns(index_ref, row, size, fold=False):
    line = index_ref[pl.ds(row, 1), :]
    if fold:
        line = jnp.where(line >= size, line - size, line)
    shape = (size, line.shape[1])
    tile = jnp.broadcast_to(line, (16, line.shape[1])).astype(I16)
    place = lax.broadcasted_iota(jnp.int32, shape, 0).astype(I16)
    return ones_where(place == jnp.concatenate([tile] * (size // 16), axis=0), shape)


def folded(column, half):
    upper = column >= float(half)
    return jnp.where(upper, column - float(half), column), upper


def side_by_side(rows):
    half = rows.shape[0] // 2
    return jnp.concatenate([rows[:half], rows[half:]], axis=1)


def stacked(pair):
    width = pair.shape[1] // 2
    return jnp.concatenate([pair[:, :width], pair[:, width:]], axis=0)


def chosen(pair, upper):
    width = pair.shape[1] // 2
    return jnp.where(upper, pair[:, width:], pair[:, :width])


def parted(rows, upper):
    zero = jnp.zeros_like(rows)
    return jnp.concatenate([jnp.where(upper, zero, rows), jnp.where(upper, rows, zero)], axis=1)


def parities():
    return (lax.rem(lax.axis_index("stream"), 2), lax.rem(lax.axis_index("cross"), 2))


def inner(axis):
    place = lax.axis_index(axis)
    return jnp.logical_and(place > 0, place < lax.axis_size(axis) - 1)


def list_order():
    odd_s, odd_c = parities()
    return (odd_s, 1 - odd_s, 2 + odd_c, 3 - odd_c)


def load_kernel(list_hbm, stale_hbm, *rest):
    count = (len(rest) - 5 - 2) // 2
    sources = rest[:count]
    outs = rest[count : count + 4]
    lists = rest[count + 4]
    kept = rest[count + 5 : 2 * count + 5]
    stale, sems = rest[2 * count + 5 :]
    copies = [
        pltpu.make_async_copy(a, b, sems.at[i])
        for i, (a, b) in enumerate(
            zip((list_hbm, stale_hbm) + sources, (lists, stale) + kept)
        )
    ]
    for copy in copies:
        copy.start()
    copies[0].wait()
    columns = [index_columns(lists, row) for row in list_order()]
    copies[1].wait()
    for column, out in zip(columns, outs):
        out[...] = mm(one_hot_rows(column, stale.shape[0]), stale[...]).astype(BF)
    for copy in copies[2:]:
        copy.wait()


def stale_kernel(list_ref, b0, b1, b2, b3, out_ref):
    total = None
    keep = (None, inner("stream"), None, inner("cross"))
    for row, part, valid in zip(list_order(), (b0, b1, b2, b3), keep):
        hot = one_hot_columns(list_ref, row, out_ref.shape[0])
        part = part[...]
        if valid is not None:
            part = jnp.where(valid, part, jnp.zeros_like(part))
        piece = mm(hot, part)
        total = piece if total is None else total + piece
    out_ref[...] = total.astype(BF)


def norm_forward(z):
    mean = jnp.mean(z, axis=-1, keepdims=True)
    centered = z - mean
    variance = jnp.mean(centered * centered, axis=-1, keepdims=True)
    inverse = lax.rsqrt(variance + EPSILON)
    return centered * inverse, jnp.broadcast_to(inverse, z.shape)


def norm_backward(slope, unit, inverse):
    first = jnp.mean(slope, axis=-1, keepdims=True)
    second = jnp.mean(slope * unit, axis=-1, keepdims=True)
    return inverse * (slope - first - unit * second)


def silu_pair(v):
    sig = 0.5 * jnp.tanh(0.5 * v) + 0.5
    hidden = v * sig
    return hidden, sig + hidden * (1.0 - sig)


def main_kernel(
    count_ref,
    latents,
    h0,
    h1,
    h2,
    h3,
    edges,
    senders,
    receivers,
    node_cot,
    edge_cot,
    edge_first,
    edge_bias,
    edge_second,
    edge_gain,
    node_first,
    node_bias,
    node_second,
    node_gain,
    new_latents,
    latent_grads,
    edge_grads,
    g0,
    g1,
    g2,
    g3,
    packed,
    table,
    hot_recv,
    turn_recv,
    turn_send,
    joined,
    hidden_s,
    slope_s,
    unit_s,
    inverse_s,
    upper_send,
    upper_recv,
    alive_edges,
    dz_s,
    dpre_s,
    dpre_send,
    dpre_recv,
    latent_out,
    grad_out,
    edge_out,
    sems,
):
    n, w = latents.shape
    e = edges.shape[0]
    t = table.shape[0]
    depth = h0.shape[0]
    chunk = e // 2
    total = count_ref[0]
    table[:n] = latents[...]
    odd_s, odd_c = parities()
    for i, (near, far, odd, axis) in enumerate(
        ((h0, h1, odd_s, "stream"), (h2, h3, odd_c, "cross"))
    ):
        place = lax.axis_index(axis)
        a, b = (near[...], far[...])
        zero = jnp.zeros_like(a)
        before = jnp.where(place > 0, jnp.where(odd == 1, a, b), zero)
        after = jnp.where(place < lax.axis_size(axis) - 1, jnp.where(odd == 1, b, a), zero)
        at = n + 2 * i * depth
        table[at : at + depth] = before
        table[at + depth : at + 2 * depth] = after
    gain = edge_gain[...]

    for c in range(e // chunk):
        rows = slice(c * chunk, (c + 1) * chunk)
        for b in range(chunk // w):
            row = c * (chunk // w) + b
            part = slice(row * w, (row + 1) * w)
            column, upper = folded(index_columns(senders, row), t // 2)
            found = mm(one_hot_rows(column, t // 2), side_by_side(table))
            joined[part, :w] = chosen(found, upper).astype(BF)
            upper_send[part] = jnp.where(upper, 1.0, 0.0).astype(BF)
            column, upper = folded(index_columns(receivers, row), n // 2)
            hot = one_hot_rows(column, n // 2)
            hot_recv[part] = hot
            found = mm(hot, side_by_side(latents))
            joined[part, w:] = chosen(found, upper).astype(BF)
            upper_recv[part] = jnp.where(upper, 1.0, 0.0).astype(BF)
            turn_send[:, part] = one_hot_columns(senders, row, t // 2, True)
            turn_recv[:, part] = one_hot_columns(receivers, row, n // 2, True)
        edge = edges[rows]
        pre = mm(edge, edge_first[:w]) + mm(joined[rows], edge_first[w:]) + edge_bias[...]
        hidden, slope = silu_pair(pre)
        hidden = hidden.astype(BF)
        hidden_s[rows] = hidden
        slope_s[rows] = slope
        unit, inverse = norm_forward(mm(hidden, edge_second[...]))
        unit_s[rows] = unit
        inverse_s[rows] = inverse
        place = lax.broadcasted_iota(jnp.int32, (chunk, w), 0) + c * chunk
        fresh = (edge.astype(F32) + unit * gain).astype(BF)
        fresh = jnp.where(place < total, fresh, jnp.zeros_like(fresh))
        alive_edges[rows] = parted(fresh, upper_recv[rows] > 0)

    aggregate = stacked(mm(turn_recv[...], alive_edges[...])).astype(BF)
    own = latents[...]
    hidden, slope = silu_pair(
        mm(jnp.concatenate([own, aggregate], axis=1), node_first[...]) + node_bias[...]
    )
    hidden = hidden.astype(BF)
    unit, inverse = norm_forward(mm(hidden, node_second[...]))
    latent_out[...] = (own.astype(F32) + unit * node_gain[...]).astype(BF)
    send_latents = pltpu.make_async_copy(latent_out, new_latents, sems.at[0])
    send_latents.start()
    ncot = node_cot[...].astype(F32)
    node_gain_grad = jnp.sum(ncot * unit, axis=0, keepdims=True)
    dz = norm_backward(ncot * node_gain[...], unit, inverse).astype(BF)
    dpre = mm_nt(dz, node_second[...]) * slope
    node_bias_grad = jnp.sum(dpre, axis=0, keepdims=True)
    dpre = dpre.astype(BF)
    down = mm_nt(dpre, node_first[...])
    d_aggregate = side_by_side(down[:, w:].astype(BF))
    latent_part = ncot + down[:, :w]
    at = 4 * w
    packed[at : at + w] = mm_tn(own, dpre).astype(BF)
    packed[at + w : at + 2 * w] = mm_tn(aggregate, dpre).astype(BF)
    packed[at + 2 * w : at + 3 * w] = mm_tn(hidden, dz).astype(BF)

    bias_grad = jnp.zeros((1, w), F32)
    gain_grad = jnp.zeros((1, w), F32)
    for c in range(e // chunk):
        rows = slice(c * chunk, (c + 1) * chunk)
        place = lax.broadcasted_iota(jnp.int32, (chunk, w), 0) + c * chunk
        alive = place < total
        upper = upper_recv[rows] > 0
        passed = chosen(mm(hot_recv[rows], d_aggregate), upper)
        cot = edge_cot[rows].astype(F32) + jnp.where(alive, passed, 0.0)
        live = jnp.where(alive, cot, 0.0)
        unit = unit_s[rows]
        gain_grad = gain_grad + jnp.sum(live * unit, axis=0, keepdims=True)
        dz = norm_backward(live * gain, unit, inverse_s[rows]).astype(BF)
        dz_s[rows] = dz
        dpre = mm_nt(dz, edge_second[...]) * slope_s[rows]
        bias_grad = bias_grad + jnp.sum(dpre, axis=0, keepdims=True)
        dpre = dpre.astype(BF)
        dpre_s[rows] = dpre
        dpre_send[rows] = parted(dpre, upper_send[rows] > 0)
        dpre_recv[rows] = parted(dpre, upper)
        edge_out[rows] = (cot + mm_nt(dpre, edge_first[:w])).astype(BF)
    send_edges = pltpu.make_async_copy(edge_out, edge_grads, sems.at[1])
    send_edges.start()

    from_send = stacked(mm(turn_send[...], dpre_send[...])).astype(BF)
    from_recv = stacked(mm(turn_recv[...], dpre_recv[...])).astype(BF)
    back = mm_nt(from_send, edge_first[w : 2 * w])
    grad_out[...] = (latent_part + back[:n] + mm_nt(from_recv, edge_first[2 * w :])).astype(BF)
    send_grads = pltpu.make_async_copy(grad_out, latent_grads, sems.at[2])
    send_grads.start()
    for i, (near, far, odd) in enumerate(((g0, g1, odd_s), (g2, g3, odd_c))):
        at = n + 2 * i * depth
        before = back[at : at + depth]
        after = back[at + depth : at + 2 * depth]
        near[...] = jnp.where(odd == 1, before, after).astype(BF)
        far[...] = jnp.where(odd == 1, after, before).astype(BF)

    dpre = dpre_s[...]
    packed[:w] = mm_tn(edges[...], dpre).astype(BF)
    packed[w : 3 * w] = mm_tn(joined[...], dpre).astype(BF)
    packed[3 * w : 4 * w] = mm_tn(hidden_s[...], dz_s[...]).astype(BF)
    tail = jnp.concatenate(
        [
            bias_grad,
            gain_grad,
            node_bias_grad,
            node_gain_grad,
            jnp.zeros((packed.shape[0] - 7 * w - 4, w), F32),
        ],
        axis=0,
    )
    packed[7 * w :] = tail.astype(BF)
    send_latents.wait()
    send_edges.wait()
    send_grads.wait()


def final_kernel(limit, mine, other, *outs):
    swap = half_of() == 1
    a, b = (mine[...].astype(F32), other[...].astype(F32))
    low = jnp.where(swap, b, a)
    high = jnp.where(swap, a, b)
    squares = jnp.sum(a * a + b * b)
    factor = jnp.minimum(1.0, limit * lax.rsqrt(jnp.full((1, a.shape[1]), squares, F32)))
    full = jnp.concatenate([low, high], axis=0) * factor
    ef, eb, es, eg, nf, nb, ns, ng = outs
    at = 0
    for out in (ef, es, nf, ns, eb, eg, nb, ng):
        out[...] = full[at : at + out.shape[0]]
        at += out.shape[0]


VM = pl.BlockSpec(memory_space=pltpu.VMEM)
SM = pl.BlockSpec(memory_space=pltpu.SMEM)
HB = pl.BlockSpec(memory_space=pltpu.HBM)


def call(kernel, outs, scratch=(), specs=None, out_specs=None):
    return pl.pallas_call(
        kernel,
        out_shape=outs,
        in_specs=specs,
        out_specs=out_specs or jax.tree.map(lambda _: VM, outs),
        scratch_shapes=list(scratch),
        compiler_params=pltpu.CompilerParams(vmem_limit_bytes=VMEM_LIMIT),
    )


def flip(axis, bit):
    return [(i, i ^ bit) for i in range(lax.axis_size(axis))]


def pair_sum(parts):
    parts = [p.astype(F32) for p in parts]
    while len(parts) > 1:
        parts = [parts[i] + parts[i + 1] for i in range(0, len(parts), 2)]
    return parts[0].astype(BF)


def level_flip(mask):
    stream, cross = (lax.axis_size("stream"), lax.axis_size("cross"))
    turn = mask >> 1 & 1
    return [
        (s * cross + c, (s ^ turn) * cross + (c ^ mask)) for s in range(stream) for c in range(cross)
    ]


def level_exchange(value, bits):
    out = [value]
    for m in range(1, 1 << len(bits)):
        mask = sum(bits[j] for j in range(len(bits)) if m >> j & 1)
        out.append(lax.ppermute(value, ("stream", "cross"), level_flip(mask)))
    return out


def exchange(value, axis, bits):
    out = [value]
    for m in range(1, 1 << len(bits)):
        mask = sum(bits[j] for j in range(len(bits)) if m >> j & 1)
        out.append(lax.ppermute(value, axis, flip(axis, mask)))
    return out


def scatter_sum(value, axis, masks, spot):
    radix = len(masks) + 1
    blocks = value.reshape((radix, value.shape[0] // radix) + value.shape[1:])
    got = [lax.dynamic_index_in_dim(blocks, spot, 0, False)]
    for k, mask in enumerate(masks):
        block = lax.dynamic_index_in_dim(blocks, spot ^ (k + 1), 0, False)
        got.append(lax.ppermute(block, axis, flip(axis, mask)))
    return got


def gather_back(value, axis, masks, spot):
    stack = jnp.stack([value] + [lax.ppermute(value, axis, flip(axis, m)) for m in masks])
    return jnp.concatenate(
        [lax.dynamic_index_in_dim(stack, spot ^ k, 0, False) for k in range(len(masks) + 1)],
        axis=0,
    )


QUAD = (3, 4, 7)


def half_of():
    place, level = (lax.axis_index("stream"), lax.axis_index("cross"))
    return lax.rem(place, 2) ^ lax.rem(place // 2, 2) ^ lax.rem(level // 2, 2)


def quarter_of(axis):
    return lax.rem(lax.axis_index(axis) // 2, 4)


def together(first, *rest):
    return lax.optimization_barrier((first,) + rest)


def odd_exchange(value, axis):
    stream, cross = (lax.axis_size("stream"), lax.axis_size("cross"))
    pairs = []
    for s in range(stream):
        for c in range(cross):
            place, size = (s, stream) if axis == "stream" else (c, cross)
            to = place + 1 if place % 2 else place - 1
            if axis == "stream":
                peer = (to, c) if 0 <= to < size else (s, c ^ 1)
            else:
                peer = (s, to) if 0 <= to < size else (s ^ 1, c)
            pairs.append((s * cross + c, peer[0] * cross + peer[1]))
    return lax.ppermute(value, ("stream", "cross"), pairs)


def reduce_all(value, near_s, far_s, near_c, far_c):
    stream, cross = (lax.axis_size("stream"), lax.axis_size("cross"))
    half, quarter = (half_of(), quarter_of("stream"))
    blocks = value.reshape((2, value.shape[0] // 2, value.shape[1]))
    mine = lax.dynamic_index_in_dim(blocks, half, 0, False)
    give = lax.dynamic_index_in_dim(blocks, 1 - half, 0, False)
    back_c = lax.ppermute(near_c, "cross", flip("cross", 1))
    got = lax.ppermute(jnp.concatenate([give, near_s]), "stream", flip("stream", 1))
    value = pair_sum([mine, got[: mine.shape[0]]])
    back_s = got[mine.shape[0] :]
    value, far_c = together(value, far_c)
    back_d = odd_exchange(far_c, "cross")
    parts, back_c = together(scatter_sum(value, "stream", QUAD, quarter), back_c)
    value = pair_sum(parts)
    low = 8
    while low < stream:
        value = pair_sum(exchange(value, "stream", [low]))
        low *= 2
    value, far_s = together(value, far_s)
    parts = level_exchange(value, [1, 2])
    back_b = odd_exchange(far_s, "stream")
    parts, back_d, back_b = together(parts, back_d, back_b)
    value = pair_sum(parts)
    low = 4
    while low < cross:
        value = pair_sum(level_exchange(value, [low, 2 * low] if 2 * low < cross else [low]))
        low *= 4
    value = gather_back(value, "stream", QUAD, quarter)
    return (value, (back_s, back_b, back_c, back_d))


def per_device(
    latents,
    stale_latents,
    edge_latents,
    senders,
    receivers,
    edge_count,
    send_list,
    node_cotangent,
    edge_cotangent,
    edge_first,
    edge_bias,
    edge_second,
    edge_gain,
    node_first,
    node_bias,
    node_second,
    node_gain,
):
    n, w = latents.shape
    e = edge_latents.shape[0]
    depth = send_list.shape[2]
    lists = send_list[0]

    sources = (
        latents,
        edge_latents,
        senders.reshape(e // w, w),
        receivers.reshape(e // w, w),
        node_cotangent,
        edge_cotangent,
        edge_first,
        edge_bias.reshape(1, w),
        edge_second,
        edge_gain.reshape(1, w),
        node_first,
        node_bias.reshape(1, w),
        node_second,
        node_gain.reshape(1, w),
    )
    loaded = call(
        load_kernel,
        (jax.ShapeDtypeStruct((depth, w), BF),) * 4
        + (jax.ShapeDtypeStruct(lists.shape, lists.dtype),)
        + tuple(jax.ShapeDtypeStruct(x.shape, x.dtype) for x in sources),
        scratch=(
            pltpu.VMEM((n, w), BF),
            pltpu.SemaphoreType.DMA((2 + len(sources),)),
        ),
        specs=[HB] * (2 + len(sources)),
    )(*(pltpu.with_memory_space_constraint(x, pltpu.HBM) for x in (lists, stale_latents) + sources))
    picked, lists, kept = (loaded[:4], loaded[4], loaded[5:])
    near_s = lax.ppermute(picked[0], "stream", flip("stream", 1))
    far_s = odd_exchange(picked[1], "stream")
    near_c = lax.ppermute(picked[2], "cross", flip("cross", 1))
    far_c = odd_exchange(picked[3], "cross")
    halo = (near_s, far_s, near_c, far_c)
    table = n + 4 * depth

    def shape(rows, kind=BF):
        return jax.ShapeDtypeStruct((rows, w), kind)

    new_latents, latent_grads, edge_grads, g0, g1, g2, g3, packed = call(
        main_kernel,
        (shape(n), shape(n), shape(e)) + (shape(depth),) * 4 + (shape(-(-(7 * w + 4) // 64) * 64),),
        scratch=(
            pltpu.VMEM((table, w), BF),
            pltpu.VMEM((e, n // 2), BF),
            pltpu.VMEM((n // 2, e), BF),
            pltpu.VMEM((table // 2, e), BF),
            pltpu.VMEM((e, 2 * w), BF),
            pltpu.VMEM((e, w), BF),
            pltpu.VMEM((e, w), F32),
            pltpu.VMEM((e, w), F32),
            pltpu.VMEM((e, w), F32),
            pltpu.VMEM((e, w), BF),
            pltpu.VMEM((e, w), BF),
            pltpu.VMEM((e, 2 * w), BF),
            pltpu.VMEM((e, w), BF),
            pltpu.VMEM((e, w), BF),
            pltpu.VMEM((e, 2 * w), BF),
            pltpu.VMEM((e, 2 * w), BF),
            pltpu.VMEM((n, w), BF),
            pltpu.VMEM((n, w), BF),
            pltpu.VMEM((e, w), BF),
            pltpu.SemaphoreType.DMA((3,)),
        ),
        specs=[SM] + [VM] * 18,
        out_specs=(HB,) * 3 + (VM,) * 5,
    )(
        edge_count, kept[0], *halo, *kept[1:]
    )
    part, returned = reduce_all(packed, g0, g1, g2, g3)
    stale_grads = call(stale_kernel, shape(n), specs=[VM] * 5)(lists, *returned)
    other = lax.ppermute(part, "stream", flip("stream", 1))
    sizes = (3 * w * w, w, w * w, w, 2 * w * w, w, w * w, w)
    limit = math.sqrt(sum(sizes))
    clipped = call(
        functools.partial(final_kernel, limit),
        tuple(shape(s // w, F32) for s in sizes),
        specs=[VM, VM],
    )(part, other)
    clipped = tuple(c.reshape(w) if s == w else c for c, s in zip(clipped, sizes))
    return (new_latents, latent_grads, stale_grads, edge_grads) + clipped


def solution(mesh):
    shard = P(("stream", "cross"))
    rows = P(("stream", "cross"), None)
    in_specs = (rows, rows, rows, shard, shard, shard, P(("stream", "cross"), None, None), rows, rows)
    in_specs = in_specs + (P(),) * 8
    out_specs = (rows,) * 4 + (P(),) * 8
    return jax.shard_map(
        per_device, mesh=mesh, in_specs=in_specs, out_specs=out_specs, check_vma=False
    )
```
